32 devices in a mesh: tile: 2 (over y), wave: 16 (over z, x, core).
Axes of the slice: x: 2, y: 2, z: 4, core: 2. Of those that a mesh axis runs over, the one named last changes fastest.
Arguments:
- frames: float32 [4, 1024, 4096], P(None, ('tile', 'wave')), parts along dimension 1, may hold values from -6 to 6
- inverse_var: float32 [4, 1024, 4096], P(None, ('tile', 'wave')), parts along dimension 1, may hold values from 0.2 to 240
- masked: int32 [4, 1024, 4096], P(None, ('tile', 'wave')), parts along dimension 1, may hold values 0 or 1
- psf_band: float32 [4, 1024, 16], P(None, ('tile', 'wave')), parts along dimension 1, may hold values from 0.02 to 0.2
- offsets: int32 [32], P(('tile', 'wave')), parts along dimension 0, may hold values from 18 to 31
- starts: int32 [32, 500], P(('tile', 'wave')), parts along dimension 0, may hold values from 0 to 3995, as said below
- profile: float32 [32, 12, 500], P(('tile', 'wave')), parts along dimension 0, may hold values from 0.05 to 0.5
- flux_start: float32 [1024, 500], P(('tile', 'wave')), parts along dimension 0, may hold values from -3 to 3
Outputs:
- solution: float32 [1024, 500], P(('tile', 'wave')), parts along dimension 0
- residual: float32 [1024, 500], P(('tile', 'wave')), parts along dimension 0
The draws below stay inside these ranges and needn't reach their ends.
There are 2 independent parts, one for each index of `tile`. The reference program is written for one: setup_inputs(seed, part) draws one part's arguments, and reference() takes and returns one part's arrays. A program takes and returns all parts, laid end to end along the dimension named above; each array names one. Nothing has to cross between parts.
Inputs may be any that keep to these rules, and one draw needn't show every extreme that they name: In every slab, fiber k's trace starts at a column from 8k to 8k + 3, so the fibers lie in order, 8 columns apart give or take 3, and neighbouring profiles intersect.
All inputs are finite; a program needn't handle non-finite values. No bound on the sum of `masked` on one device may be relied on, other than what follows from the above.
Results may differ from the reference program's by a relative error of at most 0.0003.
Values sent between devices are 32-bit elements; how exact they have to be, the bound alone decides.
No kernel may reach another device: no remote copies, remote signals or barrier semaphores. Data moves between devices by JAX's collectives and lax.ppermute only.
A program may use at most 64 MiB of HBM per device.

```python
import math
import jax
import jax.numpy as jnp
from jax import lax

FIB = 500
COLS = 4096
EXPO = 4
SLAB_ROWS = 32
ITERS = 3
HALO = 32
BAND = 16
PW = 12
SLABS = 16
WAVES = 512


def draw_inverse_var(key, part):
    first_key, second_key = jax.random.split(jax.random.fold_in(key, 11), 2)
    row_index = jnp.arange(WAVES, dtype=jnp.float32)
    ramp = 3.0 ** (row_index / WAVES)
    row_scale = 10.0 ** jax.random.uniform(second_key, (1, WAVES, 1), jnp.float32, 0.0, 1.0)
    pixels = jnp.exp(jax.random.uniform(first_key, (EXPO, WAVES, COLS), jnp.float32, math.log(0.3), math.log(3.0)))
    return pixels * row_scale * ramp[None, :, None]


def draw_starts(key, part):
    pitch = (COLS - PW - 4) // FIB
    jitter = jax.random.randint(jax.random.fold_in(key, 23), (SLABS, FIB), 0, 4, dtype=jnp.int32)
    return jnp.arange(FIB, dtype=jnp.int32)[None, :] * pitch + jitter


def plant(array, own_key, low, high):
    place = [jax.random.randint(jax.random.fold_in(own_key, axis), (), 0, length) for axis, length in enumerate(array.shape)]
    widest = array.shape.index(max(array.shape))
    beside = place[:widest] + [(place[widest] + 1) % array.shape[widest]] + place[widest + 1:]
    return array.at[tuple(place)].set(low).at[tuple(beside)].set(high)


def block_levels(own_key, shape, cuts, least, high):
    level = 1.0
    for dim, parts in cuts:
        heights = jax.random.uniform(jax.random.fold_in(jax.random.fold_in(own_key, 6), dim), (parts,), jnp.float32, least / len(cuts), high / len(cuts))
        level = level * jnp.repeat(jnp.exp(heights), shape[dim] // parts).reshape((-1,) + (1,) * (len(shape) - 1 - dim))
    return level


def normal_values(key, shape, deviation, bound, shards=(), kind=jnp.bfloat16):
    array = jax.random.normal(key, shape, jnp.float32) * deviation
    if len(shards) > 0:
        array = block_levels(key, shape, shards, -0.22, 0.18) * array
    return jnp.clip(array, min=-bound, max=bound).astype(kind)


def setup_inputs(seed: int = 0, part: int = 0) -> dict:
    streams_of = jax.random.split(jax.random.key(seed), 9)
    own_keys = jax.random.split(jax.random.fold_in(streams_of[8], part), 9)
    return {
        "frames": normal_values(own_keys[0], (EXPO, WAVES, COLS), 1.0, 6.0, ((1, 16),), jnp.float32),
        "inverse_var": draw_inverse_var(jax.random.fold_in(jax.random.fold_in(streams_of[8], part), 71), part),
        "masked": plant((jax.random.randint(own_keys[2], (EXPO, WAVES, COLS), 0, 16) < 1).astype(jnp.int32), jax.random.fold_in(own_keys[2], 1), 0, 1),
        "psf_band": jnp.clip(jnp.exp(math.log(0.2) - 2.3025851 * jax.random.uniform(own_keys[3], (EXPO, WAVES, BAND), jnp.float32) ** block_levels(own_keys[3], (EXPO, WAVES, BAND), ((1, 16),), -0.2, 0.2)), 0.02, 0.2),
        "offsets": plant(jax.random.randint(own_keys[4], (SLABS,), HALO - BAND + 2, HALO), jax.random.fold_in(own_keys[4], 1), HALO - BAND + 2, HALO - 1).astype(jnp.int32),
        "starts": draw_starts(jax.random.fold_in(jax.random.fold_in(streams_of[8], part), 71), part),
        "profile": jnp.clip(jnp.exp(math.log(0.5) - 2.3025851 * jax.random.uniform(own_keys[6], (SLABS, PW, FIB), jnp.float32) ** block_levels(own_keys[6], (SLABS, PW, FIB), ((0, 16),), -0.2, 0.2)), 0.05, 0.5),
        "flux_start": normal_values(own_keys[7], (WAVES, FIB), 0.5, 3.0, ((0, 16),), jnp.float32),
    }


RIDGE = 0.2
PRECISE = lax.Precision.HIGHEST


def row_matrix(band_slab, offset):
    width = SLAB_ROWS + 2 * HALO
    column_index = jnp.arange(width, dtype=jnp.int32)
    row_index = jnp.arange(SLAB_ROWS, dtype=jnp.int32)
    summed = jnp.zeros((band_slab.shape[0], SLAB_ROWS, width), jnp.float32)
    for band_step in range(BAND):
        selector = (column_index[None, :] == row_index[:, None] + offset + band_step).astype(jnp.float32)
        summed = summed + band_slab[:, :, band_step][:, :, None] * selector[None, :, :]
    return summed


def column_profile(starts_row, profile_slab):
    column_index = jnp.arange(COLS, dtype=jnp.int32)[:, None]
    summed = jnp.zeros((COLS, FIB), jnp.float32)
    for column_shift in range(PW):
        selector = (column_index == starts_row[None, :] + column_shift).astype(jnp.float32)
        summed = summed + profile_slab[column_shift][None, :] * selector
    return summed


def project(extended, target, weight, rowmat, colmat):
    interior = jnp.einsum('erx,xk->erk', rowmat, extended, precision=PRECISE)
    predicted = jnp.einsum('erk,ck->erc', interior, colmat, precision=PRECISE)
    weighted = weight * (target - predicted)
    folded_back = jnp.einsum('erc,ck->erk', weighted, colmat, precision=PRECISE)
    return jnp.einsum('erx,erk->xk', rowmat, folded_back, precision=PRECISE)


def diagonal_terms(weight, rowmat, colmat):
    folded_back = jnp.einsum('erc,ck->erk', weight, colmat * colmat, precision=PRECISE)
    return jnp.einsum('erx,erk->xk', rowmat * rowmat, folded_back, precision=PRECISE)


def fold_slabs(pieces):
    width = SLAB_ROWS + 2 * HALO
    positions = (jnp.arange(SLABS, dtype=jnp.int32)[:, None] * SLAB_ROWS + jnp.arange(width, dtype=jnp.int32)[None, :]).reshape(-1)
    summed = jnp.zeros((WAVES + 2 * HALO, FIB), jnp.float32).at[positions].add(pieces.reshape(-1, FIB))
    return summed[HALO:HALO + WAVES]


def reference(frames, inverse_var, masked, psf_band, offsets, starts, profile, flux_start):
    slab_list = jnp.arange(SLABS, dtype=jnp.int32)

    def slab_inputs(slab_index):
        first_row = (slab_index * SLAB_ROWS).astype(jnp.int32)
        rowmat = row_matrix(lax.dynamic_slice_in_dim(psf_band, first_row, SLAB_ROWS, 1), offsets[slab_index])
        colmat = column_profile(starts[slab_index], profile[slab_index])
        flags = lax.dynamic_slice_in_dim(masked, first_row, SLAB_ROWS, 1).astype(jnp.float32)
        weight = lax.dynamic_slice_in_dim(inverse_var, first_row, SLAB_ROWS, 1) * (1.0 - flags)
        return first_row, rowmat, colmat, weight

    def apply_all(values, with_data):
        padded = jnp.pad(values, ((HALO, HALO), (0, 0)))

        def per_slab(slab_index):
            first_row, rowmat, colmat, weight = slab_inputs(slab_index)
            extended = lax.dynamic_slice_in_dim(padded, first_row, SLAB_ROWS + 2 * HALO, 0)
            if with_data:
                target = lax.dynamic_slice_in_dim(frames, first_row, SLAB_ROWS, 1)
            else:
                target = jnp.zeros((), jnp.float32)
            return project(extended, target, weight, rowmat, colmat)

        return fold_slabs(lax.map(per_slab, slab_list))

    def diag_slab(slab_index):
        first_row, rowmat, colmat, weight = slab_inputs(slab_index)
        return diagonal_terms(weight, rowmat, colmat)

    diagonal = fold_slabs(lax.map(diag_slab, slab_list)) + RIDGE
    residual = apply_all(flux_start, True) - RIDGE * flux_start
    solution = flux_start
    scaled = residual / diagonal
    direction = scaled
    energy = jnp.sum(residual * scaled)
    for iteration in range(ITERS):
        image_dir = RIDGE * direction - apply_all(direction, False)
        step_size = energy / jnp.sum(direction * image_dir)
        solution = solution + step_size * direction
        residual = residual - step_size * image_dir
        scaled = residual / diagonal
        energy_new = jnp.sum(residual * scaled)
        direction = scaled + (energy_new / energy) * direction
        energy = energy_new
    return solution, residual
```

```python
import functools

import jax
import jax.numpy as jnp
from jax import lax
from jax.experimental import pallas as pl
from jax.experimental.pallas import tpu as pltpu
from jax.sharding import PartitionSpec as P

SLAB_ROWS = 32
HALO = 32
BAND = 16
PW = 12
PITCH = 8
RIDGE = 0.2
GHOST = 16
EXT = SLAB_ROWS + 2 * GHOST
HALF = EXT // 2
LANES = 128
FB = 128
CB = FB * PITCH
SHIFT = 10.0
PRECISE = lax.Precision.HIGHEST
F32 = jnp.float32


def dot(a, b):
    return lax.dot_general(a, b, (((1,), (0,)), ((), ())), precision=PRECISE, preferred_element_type=F32)


def pixel_kernel(starts, profile, frames, inverse_var, masked, inv_edge, mask_edge, frames_edge,
                 t0, t1, f, lo_s, hi_s, pad_s, start_s):
    block = pl.program_id(0)
    fib = starts.shape[1]
    width = pad_s.shape[1]

    @pl.when(block == 0)
    def _():
        pad_s[...] = jnp.zeros_like(pad_s)
        pad_s[0:PW, 0:fib] = profile[0]
        start_s[...] = jnp.zeros_like(start_s)
        start_s[0:1, 0:fib] = starts[...]
        lane = lax.broadcasted_iota(jnp.int32, (1, width), 1)
        jitter = start_s[0:1, :] - PITCH * lane
        base = pad_s[...]
        local = jnp.where(jitter == 0, base, 0.0)
        for d in range(1, 4):
            local = jnp.where(jitter == d, pltpu.roll(base, d, 0), local)
        low, high = local[0:8], local[8:16]
        nxt = pltpu.roll(low, width - 1, 1)
        lo_s[0] = low
        hi_s[0] = high
        lo_s[1] = low * low
        hi_s[1] = high * high
        lo_s[2] = jnp.zeros_like(low)
        hi_s[2] = high * nxt

    cols = pl.ds(pl.multiple_of(block * FB, FB), FB)
    q = lax.broadcasted_iota(jnp.int32, (FB, 8, FB), 0)
    k = lax.broadcasted_iota(jnp.int32, (FB, 8, FB), 2)
    on, after = q == k, q == k + 1
    edge_row = lax.broadcasted_iota(jnp.int32, (FB, FB), 0)
    edge_lane = lax.broadcasted_iota(jnp.int32, (FB, FB), 1)
    edge_on = (edge_row < 8) & (edge_lane == FB - 1)

    def expand(i):
        low = lo_s[i, :, cols][None]
        high = hi_s[i, :, cols][None]
        main = jnp.where(on, low, jnp.where(after, high, 0.0)).reshape(FB * 8, FB)
        tail = jnp.where(edge_on, jnp.concatenate([hi_s[i, :, cols], jnp.zeros((FB - 8, FB), F32)], 0), 0.0)
        return main, tail

    rows = t0.shape[0]
    weight = (inverse_var[...] * (1.0 - masked[...].astype(F32))).reshape(rows, CB)
    weight_e = (inv_edge[...] * (1.0 - mask_edge[...].astype(F32))).reshape(rows, FB)
    data = weight * frames[...].reshape(rows, CB)
    data_e = weight_e * frames_edge[...].reshape(rows, FB)
    m, e = expand(1)
    t0[...] = dot(weight, m) + dot(weight_e, e)
    m, e = expand(2)
    t1[...] = dot(weight, m) + dot(weight_e, e)
    m, e = expand(0)
    f[...] = dot(data, m) + dot(data_e, e)


def tri(t0, t1, u):
    width = u.shape[1]
    return t0 * u + t1 * pltpu.roll(u, width - 1, 1) + pltpu.roll(t1 * u, 1, 1)


def split(ext, parity, send_e, send_o, at):
    low, high = ext[0:HALF], ext[HALF:EXT]
    send_e[at : at + HALF, :] = jnp.where(parity == 0, high, low)
    send_o[at : at + HALF, :] = jnp.where(parity == 0, low, high)


def joined(part, got_e, got_o, parity, at):
    e, o = got_e[at : at + HALF, :], got_o[at : at + HALF, :]
    low = jnp.where(parity == 0, o, e)
    high = jnp.where(parity == 0, e, o)
    return jnp.concatenate([part[0:HALF, :] + low, part[HALF:EXT, :] + high], 0)


def lanes_of(x):
    s = jnp.sum(x, axis=0, keepdims=True)
    total = s[:, 0:LANES]
    for i in range(1, x.shape[1] // LANES):
        total = total + s[:, i * LANES : (i + 1) * LANES]
    return total


def own(x):
    return x[GHOST : GHOST + SLAB_ROWS, :]


def first_kernel(info, band, flux, flux_e, flux_o, t0, t1, f, rowmat, rowmat_t, start_ext, part, send_e, send_o, ext_s, band_s):
    parity, offset, is_first, is_last = info[0], info[1], info[2], info[3]
    fib = flux.shape[1]
    rows = t0.shape[0]
    ext_s[...] = jnp.zeros_like(ext_s)
    e, o = flux_e[...], flux_o[...]
    ext_s[0:GHOST, 0:fib] = jnp.where(parity == 0, o, e)
    ext_s[GHOST : GHOST + SLAB_ROWS, 0:fib] = flux[...]
    ext_s[GHOST + SLAB_ROWS : EXT, 0:fib] = jnp.where(parity == 0, e, o)
    band_s[...] = jnp.zeros_like(band_s)
    band_s[:, 0:BAND] = band[...].reshape(rows, BAND)
    r = band_s[...]
    place = lax.rem(lax.broadcasted_iota(jnp.int32, r.shape, 0), SLAB_ROWS)
    bit = 1
    while bit < SLAB_ROWS:
        r = jnp.where((place & bit) != 0, pltpu.roll(r, bit, 1), r)
        bit *= 2
    r = pltpu.roll(r, offset - (HALO - GHOST), 1)
    lane = lax.broadcasted_iota(jnp.int32, r.shape, 1)
    outside = ((is_first == 1) & (lane < GHOST)) | ((is_last == 1) & (lane >= GHOST + SLAB_ROWS))
    r = jnp.where(outside, 0.0, r)
    rt = r.T[0:EXT, :]
    r = r[:, 0:EXT]
    rowmat[...] = r
    rowmat_t[...] = rt
    ext = ext_s[...]
    start_ext[...] = ext
    t = f[...] - tri(t0[...], t1[...], dot(r, ext))
    back = dot(rt, t)
    diag = dot(rt * rt, t0[...])
    part[0:EXT, :] = back
    part[EXT : 2 * EXT, :] = diag
    split(back, parity, send_e, send_o, 0)
    split(diag, parity, send_e, send_o, HALF)


def apply_rows(vec, rowmat, rowmat_t, t0, t1):
    u = dot(rowmat[...], vec)
    t = tri(t0[...], t1[...], u)
    return u, t, dot(rowmat_t[...], t)


def second_kernel(info, rowmat, rowmat_t, t0, t1, start_ext, part, got_e, got_o, diag, vec, mom, part_out, send_e, send_o):
    parity = info[0]
    res = joined(part[0:EXT, :], got_e, got_o, parity, 0) - RIDGE * start_ext[...]
    d = joined(part[EXT : 2 * EXT, :], got_e, got_o, parity, HALF) + RIDGE
    p = res / d
    diag[...] = d
    vec[...] = p
    mom[...] = jnp.zeros_like(mom)
    mom[0:1, :] = lanes_of(own(p) * own(res))
    _, _, back = apply_rows(p, rowmat, rowmat_t, t0, t1)
    part_out[...] = back
    split(back, parity, send_e, send_o, 0)


def next_kernel(step, copies, info, rowmat, rowmat_t, t0, t1, diag, before, mom, part, got_e, got_o, vec, mom_out, part_out, send_e, send_o):
    parity = info[0]
    prev = before[...]
    d = diag[...]
    image = joined(part, got_e, got_o, parity, 0) + RIDGE * prev
    p = image / d - SHIFT * prev
    vec[...] = p
    scaled = own(d) * own(p)
    u, t, back = apply_rows(p, rowmat, rowmat_t, t0, t1)
    part_out[...] = back
    split(back, parity, send_e, send_o, 0)
    moments = mom[...]
    row = lax.broadcasted_iota(jnp.int32, moments.shape, 0)
    new = [(2 * step - 1, lanes_of(scaled * own(prev))), (2 * step, lanes_of(scaled * own(p)))]
    if copies:
        new.append((2 * step + 1, lanes_of(u * t) + RIDGE * lanes_of(own(p) * own(p))))
    for i, value in new:
        moments = jnp.where(row == i, value, moments)
    if copies:
        mom_out[...] = jnp.broadcast_to(moments[None], mom_out.shape)
    else:
        mom_out[...] = moments


def coefficients(mom):
    mu = [mom[i : i + 1, :] for i in range(5)]
    nu = [mu[i + 1] + SHIFT * mu[i] for i in range(4)] + [mom[5:6, :]]

    def inner(p, w):
        total = None
        for i in range(len(p)):
            for j in range(len(p)):
                term = p[i] * p[j] * w[i + j]
                total = term if total is None else total + term
        return total

    one = jnp.ones_like(mu[0])
    rho, delta, energy = [one], [one], mu[0]
    chi = []
    for step in range(3):
        alpha = energy / inner(delta, nu)
        chi = [c + alpha * x for c, x in zip(chi + [0.0 * one], delta)]
        image = [SHIFT * x for x in delta] + [0.0 * one]
        image = [x + (delta[i - 1] if i else 0.0) for i, x in enumerate(image)]
        rho = [x - alpha * y for x, y in zip(rho + [0.0 * one], image)]
        if step < 2:
            fresh = inner(rho, mu)
            beta = fresh / energy
            delta = [x + beta * y for x, y in zip(rho, delta + [0.0 * one])]
            energy = fresh
    return chi, rho


def last_kernel(info, moms, diag, start_ext, p0, p1, p2, part, got_e, got_o, solution_ref, residual_ref):
    parity = info[0]
    fib = solution_ref.shape[1]
    total = jnp.sum(moms[...], axis=0)
    total = jnp.broadcast_to(jnp.sum(total, axis=1, keepdims=True), total.shape)
    chi, rho = coefficients(total)
    width = diag.shape[1]

    def wide(c):
        return jnp.concatenate([c] * (width // LANES), 1)

    chi = [wide(c) for c in chi]
    rho = [wide(c) for c in rho]
    q0, q1, q2, d = own(p0), own(p1), own(p2), own(diag)
    image = own(joined(part, got_e, got_o, parity, 0)) + RIDGE * q2
    x = own(start_ext) + chi[0] * q0 + chi[1] * q1 + chi[2] * q2
    r = d * (rho[0] * q0 + rho[1] * q1 + rho[2] * q2) + rho[3] * (image - SHIFT * (d * q2))
    solution_ref[...] = x[:, 0:fib]
    residual_ref[...] = r[:, 0:fib]


def swap(values, pairs):
    return lax.ppermute(values, "wave", pairs)


def local(frames, inverse_var, masked, psf_band, offsets, starts, profile, flux_start):
    waves = lax.axis_size("wave")
    fib = flux_start.shape[1]
    expo, slab, columns = frames.shape
    rows = expo * slab
    blocks = columns // CB
    width = blocks * FB
    index = lax.axis_index("wave")
    parity = lax.rem(index, 2)
    even = [(i, i ^ 1) for i in range(waves) if (i ^ 1) < waves]
    odd = [(i, j) for i in range(waves) for j in (((i + 1) ^ 1) - 1,) if 0 <= j < waves and j != i]
    info = jnp.stack([parity, offsets[0], (index == 0).astype(jnp.int32), (index == waves - 1).astype(jnp.int32)])

    first, last = flux_start[0:GHOST], flux_start[SLAB_ROWS - GHOST :]
    flux_o = swap(jnp.where(parity == 0, first, last), odd)
    flux_e = swap(jnp.where(parity == 0, last, first), even)

    vm = pl.BlockSpec(memory_space=pltpu.VMEM)
    sm = pl.BlockSpec(memory_space=pltpu.SMEM)

    def shape(*dims):
        return jax.ShapeDtypeStruct(dims, F32)

    main = pl.BlockSpec((expo, slab, CB), lambda b: (0, 0, b))
    edge = pl.BlockSpec((expo, slab, FB), lambda b: (0, 0, jnp.minimum((b + 1) * (CB // FB), columns // FB - 1)))
    whole2 = pl.BlockSpec((1, fib), lambda b: (0, 0))
    whole3 = pl.BlockSpec((1, PW, fib), lambda b: (0, 0, 0))
    out = pl.BlockSpec((rows, FB), lambda b: (0, b))
    t0, t1, f = pl.pallas_call(
        pixel_kernel,
        grid=(blocks,),
        in_specs=[whole2, whole3, main, main, main, edge, edge, edge],
        out_specs=[out, out, out],
        out_shape=[shape(rows, width)] * 3,
        scratch_shapes=[
            pltpu.VMEM((3, 8, width), F32),
            pltpu.VMEM((3, 8, width), F32),
            pltpu.VMEM((16, width), F32),
            pltpu.VMEM((8, width), jnp.int32),
        ],
        compiler_params=pltpu.CompilerParams(dimension_semantics=("arbitrary",)),
        name="pixels",
    )(starts, profile, frames, inverse_var, masked, inverse_var, masked, frames)

    rowmat, rowmat_t, start_ext, part, send_e, send_o = pl.pallas_call(
        first_kernel,
        in_specs=[sm] + [vm] * 7,
        out_specs=[vm] * 6,
        out_shape=[shape(rows, EXT), shape(EXT, rows), shape(EXT, width), shape(2 * EXT, width), shape(EXT, width), shape(EXT, width)],
        scratch_shapes=[pltpu.VMEM((EXT, width), F32), pltpu.VMEM((rows, LANES), F32)],
        name="first",
    )(info, psf_band, flux_start, flux_e, flux_o, t0, t1, f)
    got_o, got_e = swap(send_o, odd), swap(send_e, even)

    diag, p0, mom, part, send_e, send_o = pl.pallas_call(
        second_kernel,
        in_specs=[sm] + [vm] * 8,
        out_specs=[vm] * 6,
        out_shape=[shape(EXT, width), shape(EXT, width), shape(8, LANES), shape(EXT, width), shape(HALF, width), shape(HALF, width)],
        name="second",
    )(info, rowmat, rowmat_t, t0, t1, start_ext, part, got_e, got_o)
    vectors = [p0]
    for step in (1, 2):
        got_o, got_e = swap(send_o, odd), swap(send_e, even)
        copies = waves if step == 2 else 0
        mom_shape = shape(waves, 8, LANES) if copies else shape(8, LANES)
        vec, mom, part, send_e, send_o = pl.pallas_call(
            functools.partial(next_kernel, step, copies),
            in_specs=[sm] + [vm] * 10,
            out_specs=[vm] * 5,
            out_shape=[shape(EXT, width), mom_shape, shape(EXT, width), shape(HALF, width), shape(HALF, width)],
            name=f"next{step}",
        )(info, rowmat, rowmat_t, t0, t1, diag, vectors[-1], mom, part, got_e, got_o)
        vectors.append(vec)
    got_o, got_e = swap(send_o, odd), swap(send_e, even)
    moms = lax.all_to_all(mom, "wave", 0, 0)
    return tuple(
        pl.pallas_call(
            last_kernel,
            in_specs=[sm] + [vm] * 9,
            out_specs=[vm] * 2,
            out_shape=[shape(slab, fib)] * 2,
            name="last",
        )(info, moms, diag, start_ext, *vectors, part, got_e, got_o)
    )


def solution(mesh):
    placed = (
        P(None, ("tile", "wave"), None),
        P(None, ("tile", "wave"), None),
        P(None, ("tile", "wave"), None),
        P(None, ("tile", "wave"), None),
        P(("tile", "wave")),
        P(("tile", "wave"), None),
        P(("tile", "wave"), None, None),
        P(("tile", "wave"), None),
    )
    return jax.shard_map(
        local,
        mesh=mesh,
        in_specs=placed,
        out_specs=(P(("tile", "wave"), None), P(("tile", "wave"), None)),
        check_vma=False,
    )
```

```python
import functools

import jax
import jax.numpy as jnp
from jax import lax
from jax.experimental import pallas as pl
from jax.experimental.pallas import tpu as pltpu
from jax.sharding import PartitionSpec as P

SLAB_ROWS = 32
HALO = 32
BAND = 16
PW = 12
PITCH = 8
RIDGE = 0.2
GHOST = 16
EXT = SLAB_ROWS + 2 * GHOST
HALF = EXT // 2
LANES = 128
FB = 128
CB = FB * PITCH
VMEM_LIMIT = 16 * 1024 * 1024
SHIFT = 10.0
PRECISE = lax.Precision.HIGHEST
F32 = jnp.float32
BF16 = jnp.bfloat16


def dot(a, b):
    return lax.dot_general(a, b, (((1,), (0,)), ((), ())), precision=PRECISE, preferred_element_type=F32)


def parts(x):
    high = x.astype(BF16)
    rest = x - high.astype(F32)
    mid = rest.astype(BF16)
    return high, mid, (rest - mid.astype(F32)).astype(BF16)


def mm(a, b):
    return lax.dot_general(a, b, (((1,), (0,)), ((), ())), preferred_element_type=F32)


def row_matrix(rt, offset):
    index = lax.axis_index("wave")
    place = lax.rem(lax.broadcasted_iota(jnp.int32, rt.shape, 1), SLAB_ROWS) + (offset - (HALO - GHOST))
    bit = 1
    while bit < EXT:
        rt = jnp.where((place & bit) != 0, pltpu.roll(rt, bit, 0), rt)
        bit *= 2
    level = lax.broadcasted_iota(jnp.int32, rt.shape, 0)
    outside = ((index == 0) & (level < GHOST)) | ((index == lax.axis_size("wave") - 1) & (level >= GHOST + SLAB_ROWS))
    return jnp.where(outside, 0.0, rt)


def pixel_kernel(offsets, starts, profile, band, frames, inverse_var, masked, t0, t1, f, rowmat, rowmat_t,
                 frames_s, inv_s, mask_s, sems, starts_s, profile_s, bands_s, side_sems, pad_s, start_s, where_s, band_s):
    fib = starts.shape[1]
    rows, width = t0.shape
    sides = [
        pltpu.make_async_copy(src, dst, side_sems.at[i])
        for i, (src, dst) in enumerate(((starts, starts_s), (profile, profile_s), (band, bands_s)))
    ]
    for c in sides:
        c.start()
    blocks = width // FB
    copies = []
    for b in range(blocks):
        cols = pl.ds(b * CB, CB)
        copies.append([
            pltpu.make_async_copy(src.at[:, :, cols], dst.at[:, :, cols], sems.at[b, i])
            for i, (src, dst) in enumerate(((inverse_var, inv_s), (masked, mask_s), (frames, frames_s)))
        ])
    for group in copies:
        for c in group:
            c.start()

    pad_s[...] = jnp.zeros_like(pad_s)
    start_s[...] = jnp.zeros_like(start_s)
    band_s[...] = jnp.zeros_like(band_s)
    group = lax.broadcasted_iota(jnp.int32, (FB * 8, FB), 0) // 8
    fiber = lax.broadcasted_iota(jnp.int32, (FB * 8, FB), 1)
    where_s[...] = (group - fiber).astype(F32).astype(BF16)
    for c in sides:
        c.wait()
    for i in range(rows // SLAB_ROWS):
        band_s[0:BAND, i * SLAB_ROWS : (i + 1) * SLAB_ROWS] = bands_s[i]
    rt = row_matrix(band_s[...], offsets[0])
    rowmat_t[...] = rt
    rowmat[...] = rt.T
    for j in range(PW):
        pad_s[j : j + 1, 0:fib] = profile_s[j]
    start_s[0:1, 0:fib] = starts_s[...]
    lane = lax.broadcasted_iota(jnp.int32, (1, width), 1)
    jitter = start_s[0:1, :] - PITCH * lane
    base = pad_s[...]
    local = jnp.where(jitter == 0, base, 0.0)
    for d in range(1, 4):
        local = jnp.where(jitter == d, pltpu.roll(base, d, 0), local)
    low, high = local[0:8], local[8:16]
    nxt = pltpu.roll(low, width - 1, 1)

    def twice(x):
        return [jnp.concatenate([p.astype(F32)] * 2, 0).astype(BF16) for p in parts(x)]

    c_low, c_high = twice(low), twice(high)
    s_low, s_high = twice(low * low), twice(high * high)
    n_high = twice(high * nxt)
    edge_row = lax.broadcasted_iota(jnp.int32, (FB, FB), 0)
    edge_lane = lax.broadcasted_iota(jnp.int32, (FB, FB), 1)
    edge_on = ((edge_row < 8) & (edge_lane == FB - 1)).astype(F32).astype(BF16)
    zero = jnp.zeros((), BF16)

    def tall(x, cols, n):
        return jnp.broadcast_to(x[:, cols][None], (n // 16, 16, FB)).reshape(n, FB)

    def weights(c0, n):
        keep = 1.0 - mask_s[:, :, c0 : c0 + n].astype(F32)
        w = (inv_s[:, :, c0 : c0 + n] * keep).reshape(rows, n)
        return w, w * frames_s[:, :, c0 : c0 + n].reshape(rows, n)

    for c in copies[0]:
        c.wait()
    for b in range(blocks):
        cols = slice(b * FB, (b + 1) * FB)
        place = where_s[...]
        on, after = place == zero, place == jnp.ones((), BF16)

        def both(lows, highs):
            return [jnp.where(on, tall(x, cols, CB), jnp.where(after, tall(y, cols, CB), zero)) for x, y in zip(lows, highs)]

        square = both(s_low, s_high)
        cross = [jnp.where(after, tall(y, cols, CB), zero) for y in n_high]
        plain = both(c_low, c_high)
        pair = [jnp.concatenate([x, y], 1) for x, y in zip(square, cross)]
        w, v = weights(b * CB, CB)
        w = parts(w)
        v = parts(v)

        def products(w, v, pair, plain):
            t = mm(w[0], pair[0]) + mm(w[0], pair[1]) + mm(w[1], pair[0])
            t = t + mm(w[1], pair[1]) + mm(w[0], pair[2]) + mm(w[2], pair[0])
            two = jnp.concatenate(plain[0:2], 1)
            g = mm(v[0], two) + mm(v[1], two)
            g = g[:, 0:FB] + g[:, FB:] + mm(v[2], plain[0]) + mm(v[0], plain[2])
            return t[:, 0:FB], t[:, FB:], g

        tt, cc, gg = products(w, v, pair, plain)
        if b + 1 < blocks:
            for c in copies[b + 1]:
                c.wait()
            w, v = weights((b + 1) * CB, FB)
            edge_pair = [jnp.concatenate([tall(x, cols, FB) * edge_on, tall(y, cols, FB) * edge_on], 1) for x, y in zip(s_high, n_high)]
            edge_plain = [tall(x, cols, FB) * edge_on for x in c_high]
            et, ec, eg = products(parts(w), parts(v), edge_pair, edge_plain)
            tt, cc, gg = tt + et, cc + ec, gg + eg
        t0[:, cols] = tt
        t1[:, cols] = cc
        f[:, cols] = gg


def tri(t0, t1, u):
    width = u.shape[1]
    return t0 * u + t1 * pltpu.roll(u, width - 1, 1) + pltpu.roll(t1 * u, 1, 1)


def split(ext, parity, send_e, send_o, at):
    low, high = ext[0:HALF], ext[HALF:EXT]
    send_e[at : at + HALF, :] = jnp.where(parity == 0, high, low)
    send_o[at : at + HALF, :] = jnp.where(parity == 0, low, high)


def joined(part, got_e, got_o, parity, at):
    e, o = got_e[at : at + HALF, :], got_o[at : at + HALF, :]
    low = jnp.where(parity == 0, o, e)
    high = jnp.where(parity == 0, e, o)
    return jnp.concatenate([part[0:HALF, :] + low, part[HALF:EXT, :] + high], 0)


def lanes_of(x):
    s = jnp.sum(x, axis=0, keepdims=True)
    total = s[:, 0:LANES]
    for i in range(1, x.shape[1] // LANES):
        total = total + s[:, i * LANES : (i + 1) * LANES]
    return total


def own(x):
    return x[GHOST : GHOST + SLAB_ROWS, :]


def first_kernel(flux, flux_e, flux_o, t0, t1, f, rowmat, rowmat_t, start_ext, part, send_e, send_o, ext_s):
    parity = lax.rem(lax.axis_index("wave"), 2)
    fib = flux.shape[1]
    ext_s[...] = jnp.zeros_like(ext_s)
    cut = SLAB_ROWS - GHOST
    e, o = flux_e[...], flux_o[...]
    ext_s[0:GHOST, 0:fib] = jnp.where(parity == 0, o[cut:], e[cut:])
    ext_s[GHOST : GHOST + SLAB_ROWS, 0:fib] = flux[...]
    ext_s[GHOST + SLAB_ROWS : EXT, 0:fib] = jnp.where(parity == 0, e[0:GHOST], o[0:GHOST])
    r, rt = rowmat[...], rowmat_t[...]
    ext = ext_s[...]
    start_ext[...] = ext
    t = f[...] - tri(t0[...], t1[...], dot(r, ext))
    back = dot(rt, t)
    diag = dot(rt * rt, t0[...])
    part[0:EXT, :] = back
    part[EXT : 2 * EXT, :] = diag
    split(back, parity, send_e, send_o, 0)
    split(diag, parity, send_e, send_o, HALF)


def apply_rows(vec, rowmat, rowmat_t, t0, t1):
    u = dot(rowmat[...], vec)
    t = tri(t0[...], t1[...], u)
    return u, t, dot(rowmat_t[...], t)


def second_kernel(rowmat, rowmat_t, t0, t1, start_ext, part, got_e, got_o, diag, vec, mom, part_out, send_e, send_o):
    parity = lax.rem(lax.axis_index("wave"), 2)
    res = joined(part[0:EXT, :], got_e, got_o, parity, 0) - RIDGE * start_ext[...]
    d = joined(part[EXT : 2 * EXT, :], got_e, got_o, parity, HALF) + RIDGE
    p = res / d
    diag[...] = d
    vec[...] = p
    mom[...] = jnp.zeros_like(mom)
    mom[0:1, :] = lanes_of(own(p) * own(res))
    _, _, back = apply_rows(p, rowmat, rowmat_t, t0, t1)
    part_out[...] = back
    split(back, parity, send_e, send_o, 0)


def next_kernel(step, copies, rowmat, rowmat_t, t0, t1, diag, before, mom, part, got_e, got_o, vec, mom_out, part_out, send_e, send_o):
    parity = lax.rem(lax.axis_index("wave"), 2)
    prev = before[...]
    d = diag[...]
    image = joined(part, got_e, got_o, parity, 0) + RIDGE * prev
    p = image / d - SHIFT * prev
    vec[...] = p
    scaled = own(d) * own(p)
    u, t, back = apply_rows(p, rowmat, rowmat_t, t0, t1)
    part_out[...] = back
    split(back, parity, send_e, send_o, 0)
    moments = mom[...]
    row = lax.broadcasted_iota(jnp.int32, moments.shape, 0)
    new = [(2 * step - 1, lanes_of(scaled * own(prev))), (2 * step, lanes_of(scaled * own(p)))]
    if copies:
        new.append((2 * step + 1, lanes_of(u * t) + RIDGE * lanes_of(own(p) * own(p))))
    for i, value in new:
        moments = jnp.where(row == i, value, moments)
    if copies:
        mom_out[...] = jnp.broadcast_to(moments[None], mom_out.shape)
    else:
        mom_out[...] = moments


def coefficients(mom):
    mu = [mom[i : i + 1, :] for i in range(5)]
    nu = [mu[i + 1] + SHIFT * mu[i] for i in range(4)] + [mom[5:6, :]]

    def inner(p, w):
        total = None
        for i in range(len(p)):
            for j in range(len(p)):
                term = p[i] * p[j] * w[i + j]
                total = term if total is None else total + term
        return total

    one = jnp.ones_like(mu[0])
    rho, delta, energy = [one], [one], mu[0]
    chi = []
    for step in range(3):
        alpha = energy / inner(delta, nu)
        chi = [c + alpha * x for c, x in zip(chi + [0.0 * one], delta)]
        image = [SHIFT * x for x in delta] + [0.0 * one]
        image = [x + (delta[i - 1] if i else 0.0) for i, x in enumerate(image)]
        rho = [x - alpha * y for x, y in zip(rho + [0.0 * one], image)]
        if step < 2:
            fresh = inner(rho, mu)
            beta = fresh / energy
            delta = [x + beta * y for x, y in zip(rho, delta + [0.0 * one])]
            energy = fresh
    return chi, rho


def last_kernel(moms, diag, start_ext, p0, p1, p2, part, got_e, got_o, solution_ref, residual_ref):
    parity = lax.rem(lax.axis_index("wave"), 2)
    fib = solution_ref.shape[1]
    total = jnp.sum(moms[...], axis=0)
    total = jnp.broadcast_to(jnp.sum(total, axis=1, keepdims=True), total.shape)
    chi, rho = coefficients(total)
    width = diag.shape[1]

    def wide(c):
        return jnp.concatenate([c] * (width // LANES), 1)

    chi = [wide(c) for c in chi]
    rho = [wide(c) for c in rho]
    q0, q1, q2, d = own(p0), own(p1), own(p2), own(diag)
    image = own(joined(part, got_e, got_o, parity, 0)) + RIDGE * q2
    x = own(start_ext) + chi[0] * q0 + chi[1] * q1 + chi[2] * q2
    r = d * (rho[0] * q0 + rho[1] * q1 + rho[2] * q2) + rho[3] * (image - SHIFT * (d * q2))
    solution_ref[...] = x[:, 0:fib]
    residual_ref[...] = r[:, 0:fib]


def swap(values, pairs):
    return lax.ppermute(values, "wave", pairs)


def local(frames, inverse_var, masked, psf_band, offsets, starts, profile, flux_start):
    waves = lax.axis_size("wave")
    fib = flux_start.shape[1]
    expo, slab, columns = frames.shape
    rows = expo * slab
    blocks = columns // CB
    width = blocks * FB
    even = [(i, i ^ 1) for i in range(waves) if (i ^ 1) < waves]
    odd = [(i, j) for i in range(waves) for j in (((i + 1) ^ 1) - 1,) if 0 <= j < waves and j != i]

    flux_o, flux_e = swap(flux_start, odd), swap(flux_start, even)

    vm = pl.BlockSpec(memory_space=pltpu.VMEM)
    small = pltpu.CompilerParams(vmem_limit_bytes=VMEM_LIMIT)

    def shape(*dims):
        return jax.ShapeDtypeStruct(dims, F32)

    hb = pl.BlockSpec(memory_space=pltpu.HBM)
    sm = pl.BlockSpec(memory_space=pltpu.SMEM)
    raw = (offsets, starts, jnp.transpose(profile, (1, 0, 2)), jnp.transpose(psf_band, (0, 2, 1)), frames, inverse_var, masked)
    raw = [raw[0]] + [pltpu.with_memory_space_constraint(x, pltpu.HBM) for x in raw[1:]]
    t0, t1, f, rowmat, rowmat_t = pl.pallas_call(
        pixel_kernel,
        in_specs=[sm] + [hb] * 6,
        out_specs=[vm] * 5,
        out_shape=[shape(rows, width)] * 3 + [shape(rows, EXT), shape(EXT, rows)],
        scratch_shapes=[
            pltpu.VMEM(frames.shape, F32),
            pltpu.VMEM(frames.shape, F32),
            pltpu.VMEM(frames.shape, jnp.int32),
            pltpu.SemaphoreType.DMA((blocks, 3)),
            pltpu.VMEM((1, fib), jnp.int32),
            pltpu.VMEM((PW, 1, fib), F32),
            pltpu.VMEM((expo, BAND, slab), F32),
            pltpu.SemaphoreType.DMA((3,)),
            pltpu.VMEM((16, width), F32),
            pltpu.VMEM((8, width), jnp.int32),
            pltpu.VMEM((CB, FB), BF16),
            pltpu.VMEM((EXT, rows), F32),
        ],
        compiler_params=small,
        name="pixels",
    )(*raw)

    start_ext, part, send_e, send_o = pl.pallas_call(
        first_kernel,
        in_specs=[vm] * 8,
        out_specs=[vm] * 4,
        out_shape=[shape(EXT, width), shape(2 * EXT, width), shape(EXT, width), shape(EXT, width)],
        scratch_shapes=[pltpu.VMEM((EXT, width), F32)],
        compiler_params=small,
        name="first",
    )(flux_start, flux_e, flux_o, t0, t1, f, rowmat, rowmat_t)
    got_o, got_e = swap(send_o, odd), swap(send_e, even)

    diag, p0, mom, part, send_e, send_o = pl.pallas_call(
        second_kernel,
        in_specs=[vm] * 8,
        out_specs=[vm] * 6,
        out_shape=[shape(EXT, width), shape(EXT, width), shape(8, LANES), shape(EXT, width), shape(HALF, width), shape(HALF, width)],
        compiler_params=small,
        name="second",
    )(rowmat, rowmat_t, t0, t1, start_ext, part, got_e, got_o)
    vectors = [p0]
    for step in (1, 2):
        got_o, got_e = swap(send_o, odd), swap(send_e, even)
        copies = waves if step == 2 else 0
        mom_shape = shape(waves, 8, LANES) if copies else shape(8, LANES)
        vec, mom, part, send_e, send_o = pl.pallas_call(
            functools.partial(next_kernel, step, copies),
            in_specs=[vm] * 10,
            out_specs=[vm] * 5,
            out_shape=[shape(EXT, width), mom_shape, shape(EXT, width), shape(HALF, width), shape(HALF, width)],
            compiler_params=small,
            name=f"next{step}",
        )(rowmat, rowmat_t, t0, t1, diag, vectors[-1], mom, part, got_e, got_o)
        vectors.append(vec)
    got_o, got_e = swap(send_o, odd), swap(send_e, even)
    moms = lax.all_to_all(mom, "wave", 0, 0)
    return tuple(
        pl.pallas_call(
            last_kernel,
            in_specs=[vm] * 9,
            out_specs=[vm] * 2,
            out_shape=[shape(slab, fib)] * 2,
            compiler_params=small,
        name="last",
        )(moms, diag, start_ext, *vectors, part, got_e, got_o)
    )


def solution(mesh):
    placed = (
        P(None, ("tile", "wave"), None),
        P(None, ("tile", "wave"), None),
        P(None, ("tile", "wave"), None),
        P(None, ("tile", "wave"), None),
        P(("tile", "wave")),
        P(("tile", "wave"), None),
        P(("tile", "wave"), None, None),
        P(("tile", "wave"), None),
    )
    return jax.shard_map(
        local,
        mesh=mesh,
        in_specs=placed,
        out_specs=(P(("tile", "wave"), None), P(("tile", "wave"), None)),
        check_vma=False,
    )
```

```python
import functools

import jax
import jax.numpy as jnp
from jax import lax
from jax.experimental import pallas as pl
from jax.experimental.pallas import tpu as pltpu
from jax.sharding import PartitionSpec as P

SLAB_ROWS = 32
HALO = 32
BAND = 16
PW = 12
PITCH = 8
RIDGE = 0.2
GHOST = 16
EXT = SLAB_ROWS + 2 * GHOST
HALF = EXT // 2
LANES = 128
FB = 128
CB = FB * PITCH
VMEM_LIMIT = 16 * 1024 * 1024
SHIFT = 10.0
PRECISE = lax.Precision.HIGHEST
F32 = jnp.float32
BF16 = jnp.bfloat16


def dot(a, b):
    return lax.dot_general(a, b, (((1,), (0,)), ((), ())), precision=PRECISE, preferred_element_type=F32)


def parts(x):
    high = x.astype(BF16)
    rest = x - high.astype(F32)
    mid = rest.astype(BF16)
    return high, mid, (rest - mid.astype(F32)).astype(BF16)


def mm(a, b):
    return lax.dot_general(a, b, (((1,), (0,)), ((), ())), preferred_element_type=F32)


def row_matrix(rt, offset):
    index = lax.axis_index("wave")
    place = lax.rem(lax.broadcasted_iota(jnp.int32, rt.shape, 1), SLAB_ROWS) + (offset - (HALO - GHOST))
    bit = 1
    while bit < EXT:
        rt = jnp.where((place & bit) != 0, pltpu.roll(rt, bit, 0), rt)
        bit *= 2
    level = lax.broadcasted_iota(jnp.int32, rt.shape, 0)
    outside = ((index == 0) & (level < GHOST)) | ((index == lax.axis_size("wave") - 1) & (level >= GHOST + SLAB_ROWS))
    return jnp.where(outside, 0.0, rt)


def pixel_kernel(offsets, starts, profile, band, frames, inverse_var, masked, t0, t1, f, rowmat, rowmat_t,
                 frames_s, inv_s, mask_s, sems, starts_s, profile_s, bands_s, side_sems, pad_s, start_s, band_s):
    fib = starts.shape[1]
    rows, width = t0.shape
    side_copies = [
        pltpu.make_async_copy(src, dst, side_sems.at[i])
        for i, (src, dst) in enumerate(((starts, starts_s), (profile, profile_s), (band, bands_s)))
    ]
    for c in side_copies:
        c.start()
    blocks = width // FB
    copies = []
    for b in range(blocks):
        cols = pl.ds(b * CB, CB)
        copies.append([
            pltpu.make_async_copy(src.at[:, :, cols], dst.at[:, :, cols], sems.at[b, i])
            for i, (src, dst) in enumerate(((inverse_var, inv_s), (masked, mask_s), (frames, frames_s)))
        ])
    for c in copies[0]:
        c.start()

    pad_s[...] = jnp.zeros_like(pad_s)
    start_s[...] = jnp.zeros_like(start_s)
    band_s[...] = jnp.zeros_like(band_s)
    for c in side_copies:
        c.wait()
    for i in range(rows // SLAB_ROWS):
        band_s[0:BAND, i * SLAB_ROWS : (i + 1) * SLAB_ROWS] = bands_s[i]
    for c in copies[1]:
        c.start()
    rt = row_matrix(band_s[...], offsets[0])
    rowmat_t[...] = rt
    rowmat[...] = rt.T
    for j in range(PW):
        pad_s[j : j + 1, 0:fib] = profile_s[j]
    start_s[0:1, 0:fib] = starts_s[...]
    lane = lax.broadcasted_iota(jnp.int32, (1, width), 1)
    jitter = start_s[0:1, :] - PITCH * lane
    base = pad_s[...]
    local = jnp.where(jitter == 0, base, 0.0)
    for d in range(1, 4):
        local = jnp.where(jitter == d, pltpu.roll(base, d, 0), local)
    low, high = local[0:8], local[8:16]
    nxt = pltpu.roll(low, width - 1, 1)

    def twice(x):
        return [jnp.concatenate([p.astype(F32)] * 2, 0).astype(BF16) for p in parts(x)]

    c_low, c_high = twice(low), twice(high)
    s_low, s_high = twice(low * low), twice(high * high)
    n_high = twice(high * nxt)
    zero = jnp.zeros((16, FB), BF16)
    lane = lax.broadcasted_iota(jnp.int32, (16, FB), 1) - lax.broadcasted_iota(jnp.int32, (16, FB), 0) // 8
    lane = lane.astype(F32).astype(BF16)
    edge = (lax.broadcasted_iota(jnp.int32, (16, FB), 1) == FB - 1) & (lax.broadcasted_iota(jnp.int32, (16, FB), 0) < 8)
    edge = edge.astype(F32).astype(BF16)

    def expand(b):
        cols = slice(b * FB, (b + 1) * FB)
        cl, ch = [x[:, cols] for x in c_low], [x[:, cols] for x in c_high]
        sl, sh = [x[:, cols] for x in s_low], [x[:, cols] for x in s_high]
        nh = [x[:, cols] for x in n_high]
        square, cross, plain = ([[], [], []] for _ in range(3))
        for t in range(CB // 16):
            on = lane == jnp.asarray(2 * t, BF16)
            after = lane == jnp.asarray(2 * t - 1, BF16)
            for i in range(3):
                square[i].append(jnp.where(on, sl[i], jnp.where(after, sh[i], zero)))
                cross[i].append(jnp.where(after, nh[i], zero))
                plain[i].append(jnp.where(on, cl[i], jnp.where(after, ch[i], zero)))
        return [[jnp.concatenate(x, 0) for x in group] for group in (square, cross, plain)]

    def products(w, v, square, cross, plain):
        pair = [jnp.concatenate([x, y], 1) for x, y in zip(square, cross)]
        t = mm(jnp.concatenate(w, 0), pair[0])
        g = mm(jnp.concatenate(w[0:2], 0), pair[1])
        t = t[0:rows] + t[rows : 2 * rows] + t[2 * rows :] + g[0:rows] + g[rows:] + mm(w[0], pair[2])
        g = mm(jnp.concatenate(v, 0), jnp.concatenate(plain[0:2], 1))
        g = g[0:rows] + g[rows : 2 * rows] + g[2 * rows :]
        g = g[:, 0:FB] + g[:, FB:] + mm(v[0], plain[2])
        return t[:, 0:FB], t[:, FB:], g

    for b in range(blocks):
        for c in copies[b]:
            c.wait()
        if b + 2 < blocks:
            for c in copies[b + 2]:
                c.start()
        at = slice(b * CB, (b + 1) * CB)
        w = (inv_s[:, :, at] * (1.0 - mask_s[:, :, at].astype(F32))).reshape(rows, CB)
        v = w * frames_s[:, :, at].reshape(rows, CB)
        w, v = parts(w), parts(v)
        tt, cc, gg = products(w, v, *expand(b))
        cols = slice(b * FB, (b + 1) * FB)
        t0[:, cols] = tt
        t1[:, cols] = cc
        f[:, cols] = gg
        if b > 0:
            cols = slice((b - 1) * FB, b * FB)
            below = jnp.zeros((FB - 16, FB), BF16)

            def tip(x):
                return jnp.concatenate([x[:, cols] * edge, below], 0)

            tips = [[tip(x) for x in group] for group in (s_high, n_high, c_high)]
            tt, cc, gg = products([x[:, 0:FB] for x in w], [x[:, 0:FB] for x in v], *tips)
            t0[:, cols] += tt
            t1[:, cols] += cc
            f[:, cols] += gg


def tri(t0, t1, u):
    width = u.shape[1]
    return t0 * u + t1 * pltpu.roll(u, width - 1, 1) + pltpu.roll(t1 * u, 1, 1)


def split(ext, parity, send_e, send_o, at):
    low, high = ext[0:HALF], ext[HALF:EXT]
    send_e[at : at + HALF, :] = jnp.where(parity == 0, high, low)
    send_o[at : at + HALF, :] = jnp.where(parity == 0, low, high)


def sides(e, o):
    index, last = lax.axis_index("wave"), lax.axis_size("wave") - 1
    even = lax.rem(index, 2) == 0
    low = jnp.where(index == 0, 0.0, jnp.where(even, o, e))
    return low, jnp.where(index == last, 0.0, jnp.where(even, e, o))


def joined(part, got_e, got_o, at):
    low, high = sides(got_e[at : at + HALF, :], got_o[at : at + HALF, :])
    return jnp.concatenate([part[0:HALF, :] + low, part[HALF:EXT, :] + high], 0)


def lanes_of(x):
    s = jnp.sum(x, axis=0, keepdims=True)
    total = s[:, 0:LANES]
    for i in range(1, x.shape[1] // LANES):
        total = total + s[:, i * LANES : (i + 1) * LANES]
    return total


def own(x):
    return x[GHOST : GHOST + SLAB_ROWS, :]


def first_kernel(flux, flux_e, flux_o, t0, t1, f, rowmat, rowmat_t, start_ext, part, send_e, send_o, ext_s):
    parity = lax.rem(lax.axis_index("wave"), 2)
    fib = flux.shape[1]
    ext_s[...] = jnp.zeros_like(ext_s)
    low, high = sides(flux_e[...], flux_o[...])
    ext_s[0:GHOST, 0:fib] = low[SLAB_ROWS - GHOST :]
    ext_s[GHOST : GHOST + SLAB_ROWS, 0:fib] = flux[...]
    ext_s[GHOST + SLAB_ROWS : EXT, 0:fib] = high[0:GHOST]
    r, rt = rowmat[...], rowmat_t[...]
    ext = ext_s[...]
    start_ext[...] = ext
    t = f[...] - tri(t0[...], t1[...], dot(r, ext))
    back = dot(rt, t)
    diag = dot(rt * rt, t0[...])
    part[0:EXT, :] = back
    part[EXT : 2 * EXT, :] = diag
    split(back, parity, send_e, send_o, 0)
    split(diag, parity, send_e, send_o, HALF)


def apply_rows(vec, rowmat, rowmat_t, t0, t1):
    u = dot(rowmat[...], vec)
    t = tri(t0[...], t1[...], u)
    return u, t, dot(rowmat_t[...], t)


def second_kernel(rowmat, rowmat_t, t0, t1, start_ext, part, got_e, got_o, diag, vec, mom, part_out, send_e, send_o):
    parity = lax.rem(lax.axis_index("wave"), 2)
    res = joined(part[0:EXT, :], got_e, got_o, 0) - RIDGE * start_ext[...]
    d = joined(part[EXT : 2 * EXT, :], got_e, got_o, HALF) + RIDGE
    p = res / d
    diag[...] = d
    vec[...] = p
    mom[...] = jnp.zeros_like(mom)
    mom[0:1, :] = lanes_of(own(p) * own(res))
    _, _, back = apply_rows(p, rowmat, rowmat_t, t0, t1)
    part_out[...] = back
    split(back, parity, send_e, send_o, 0)


def next_kernel(step, copies, rowmat, rowmat_t, t0, t1, diag, before, mom, part, got_e, got_o, vec, mom_out, part_out, send_e, send_o):
    parity = lax.rem(lax.axis_index("wave"), 2)
    prev = before[...]
    d = diag[...]
    image = joined(part, got_e, got_o, 0) + RIDGE * prev
    p = image / d - SHIFT * prev
    vec[...] = p
    scaled = own(d) * own(p)
    u, t, back = apply_rows(p, rowmat, rowmat_t, t0, t1)
    part_out[...] = back
    split(back, parity, send_e, send_o, 0)
    moments = mom[...]
    row = lax.broadcasted_iota(jnp.int32, moments.shape, 0)
    new = [(2 * step - 1, lanes_of(scaled * own(prev))), (2 * step, lanes_of(scaled * own(p)))]
    if copies:
        new.append((2 * step + 1, lanes_of(u * t) + RIDGE * lanes_of(own(p) * own(p))))
    for i, value in new:
        moments = jnp.where(row == i, value, moments)
    if copies:
        mom_out[...] = jnp.broadcast_to(moments[None], mom_out.shape)
    else:
        mom_out[...] = moments


def coefficients(mom):
    mu = [mom[i : i + 1, :] for i in range(5)]
    nu = [mu[i + 1] + SHIFT * mu[i] for i in range(4)] + [mom[5:6, :]]

    def inner(p, w):
        total = None
        for i in range(len(p)):
            for j in range(len(p)):
                term = p[i] * p[j] * w[i + j]
                total = term if total is None else total + term
        return total

    one = jnp.ones_like(mu[0])
    rho, delta, energy = [one], [one], mu[0]
    chi = []
    for step in range(3):
        alpha = energy / inner(delta, nu)
        chi = [c + alpha * x for c, x in zip(chi + [0.0 * one], delta)]
        image = [SHIFT * x for x in delta] + [0.0 * one]
        image = [x + (delta[i - 1] if i else 0.0) for i, x in enumerate(image)]
        rho = [x - alpha * y for x, y in zip(rho + [0.0 * one], image)]
        if step < 2:
            fresh = inner(rho, mu)
            beta = fresh / energy
            delta = [x + beta * y for x, y in zip(rho, delta + [0.0 * one])]
            energy = fresh
    return chi, rho


def last_kernel(moms, diag, start_ext, p0, p1, p2, part, got_e, got_o, solution_ref, residual_ref):
    fib = solution_ref.shape[1]
    total = jnp.sum(moms[...], axis=0)
    total = jnp.broadcast_to(jnp.sum(total, axis=1, keepdims=True), total.shape)
    chi, rho = coefficients(total)
    width = diag.shape[1]

    def wide(c):
        return jnp.concatenate([c] * (width // LANES), 1)

    chi = [wide(c) for c in chi]
    rho = [wide(c) for c in rho]
    q0, q1, q2, d = own(p0), own(p1), own(p2), own(diag)
    image = own(joined(part, got_e, got_o, 0)) + RIDGE * q2
    x = own(start_ext) + chi[0] * q0 + chi[1] * q1 + chi[2] * q2
    r = d * (rho[0] * q0 + rho[1] * q1 + rho[2] * q2) + rho[3] * (image - SHIFT * (d * q2))
    solution_ref[...] = x[:, 0:fib]
    residual_ref[...] = r[:, 0:fib]


def partners(tiles, waves):
    even, odd = [], []
    for tile in range(tiles):
        for i in range(waves):
            here = tile * waves + i
            for found, other in ((even, i ^ 1), (odd, ((i + 1) ^ 1) - 1)):
                if 0 <= other < waves:
                    found.append((here, tile * waves + other))
                elif tile ^ 1 < tiles:
                    found.append((here, (tile ^ 1) * waves + i))
    return even, odd


def swap(values, pairs):
    return lax.ppermute(values, ("tile", "wave"), pairs)


def local(frames, inverse_var, masked, psf_band, offsets, starts, profile, flux_start):
    waves = lax.axis_size("wave")
    fib = flux_start.shape[1]
    expo, slab, columns = frames.shape
    rows = expo * slab
    blocks = columns // CB
    width = blocks * FB
    even, odd = partners(lax.axis_size("tile"), waves)
    flux_o, flux_e = swap(flux_start, odd), swap(flux_start, even)

    vm = pl.BlockSpec(memory_space=pltpu.VMEM)
    small = pltpu.CompilerParams(vmem_limit_bytes=VMEM_LIMIT)

    def shape(*dims):
        return jax.ShapeDtypeStruct(dims, F32)

    hb = pl.BlockSpec(memory_space=pltpu.HBM)
    sm = pl.BlockSpec(memory_space=pltpu.SMEM)
    raw = (offsets, starts, jnp.transpose(profile, (1, 0, 2)), jnp.transpose(psf_band, (0, 2, 1)), frames, inverse_var, masked)
    raw = [raw[0]] + [pltpu.with_memory_space_constraint(x, pltpu.HBM) for x in raw[1:]]
    t0, t1, f, rowmat, rowmat_t = pl.pallas_call(
        pixel_kernel,
        in_specs=[sm] + [hb] * 6,
        out_specs=[vm] * 5,
        out_shape=[shape(rows, width)] * 3 + [shape(rows, EXT), shape(EXT, rows)],
        scratch_shapes=[
            pltpu.VMEM(frames.shape, F32),
            pltpu.VMEM(frames.shape, F32),
            pltpu.VMEM(frames.shape, jnp.int32),
            pltpu.SemaphoreType.DMA((blocks, 3)),
            pltpu.VMEM((1, fib), jnp.int32),
            pltpu.VMEM((PW, 1, fib), F32),
            pltpu.VMEM((expo, BAND, slab), F32),
            pltpu.SemaphoreType.DMA((3,)),
            pltpu.VMEM((16, width), F32),
            pltpu.VMEM((8, width), jnp.int32),
            pltpu.VMEM((EXT, rows), F32),
        ],
        compiler_params=small,
        name="pixels",
    )(*raw)

    start_ext, part, send_e, send_o = pl.pallas_call(
        first_kernel,
        in_specs=[vm] * 8,
        out_specs=[vm] * 4,
        out_shape=[shape(EXT, width), shape(2 * EXT, width), shape(EXT, width), shape(EXT, width)],
        scratch_shapes=[pltpu.VMEM((EXT, width), F32)],
        compiler_params=small,
        name="first",
    )(flux_start, flux_e, flux_o, t0, t1, f, rowmat, rowmat_t)
    got_o, got_e = swap(send_o, odd), swap(send_e, even)

    diag, p0, mom, part, send_e, send_o = pl.pallas_call(
        second_kernel,
        in_specs=[vm] * 8,
        out_specs=[vm] * 6,
        out_shape=[shape(EXT, width), shape(EXT, width), shape(8, LANES), shape(EXT, width), shape(HALF, width), shape(HALF, width)],
        compiler_params=small,
        name="second",
    )(rowmat, rowmat_t, t0, t1, start_ext, part, got_e, got_o)
    vectors = [p0]
    for step in (1, 2):
        got_o, got_e = swap(send_o, odd), swap(send_e, even)
        copies = waves if step == 2 else 0
        mom_shape = shape(waves, 8, LANES) if copies else shape(8, LANES)
        vec, mom, part, send_e, send_o = pl.pallas_call(
            functools.partial(next_kernel, step, copies),
            in_specs=[vm] * 10,
            out_specs=[vm] * 5,
            out_shape=[shape(EXT, width), mom_shape, shape(EXT, width), shape(HALF, width), shape(HALF, width)],
            compiler_params=small,
            name=f"next{step}",
        )(rowmat, rowmat_t, t0, t1, diag, vectors[-1], mom, part, got_e, got_o)
        vectors.append(vec)
    got_o, got_e = swap(send_o, odd), swap(send_e, even)
    moms = lax.all_to_all(mom, "wave", 0, 0)
    return tuple(
        pl.pallas_call(
            last_kernel,
            in_specs=[vm] * 9,
            out_specs=[vm] * 2,
            out_shape=[shape(slab, fib)] * 2,
            compiler_params=small,
        name="last",
        )(moms, diag, start_ext, *vectors, part, got_e, got_o)
    )


def solution(mesh):
    placed = (
        P(None, ("tile", "wave"), None),
        P(None, ("tile", "wave"), None),
        P(None, ("tile", "wave"), None),
        P(None, ("tile", "wave"), None),
        P(("tile", "wave")),
        P(("tile", "wave"), None),
        P(("tile", "wave"), None, None),
        P(("tile", "wave"), None),
    )
    return jax.shard_map(
        local,
        mesh=mesh,
        in_specs=placed,
        out_specs=(P(("tile", "wave"), None), P(("tile", "wave"), None)),
        check_vma=False,
    )
```

```python
import functools

import jax
import jax.numpy as jnp
from jax import lax
from jax.experimental import pallas as pl
from jax.experimental.pallas import tpu as pltpu
from jax.sharding import PartitionSpec as P


SLAB_ROWS = 32
HALO = 32
BAND = 16
PW = 12
PITCH = 8
RIDGE = 0.2
GHOST = 16
EXT = SLAB_ROWS + 2 * GHOST
HALF = EXT // 2
LANES = 128
FB = 128
CB = FB * PITCH
VMEM_LIMIT = 16 * 1024 * 1024
SHIFT = 14.0
PRECISE = lax.Precision.HIGHEST
F32 = jnp.float32
BF16 = jnp.bfloat16


def dot(a, b):
    return lax.dot_general(a, b, (((1,), (0,)), ((), ())), precision=PRECISE, preferred_element_type=F32)


def parts(x):
    high = x.astype(BF16)
    rest = x - high.astype(F32)
    mid = rest.astype(BF16)
    return high, mid, (rest - mid.astype(F32)).astype(BF16)


def mm(a, b):
    return lax.dot_general(a, b, (((1,), (0,)), ((), ())), preferred_element_type=F32)


def row_matrix(rt, offset):
    index = lax.axis_index("wave")
    place = lax.rem(lax.broadcasted_iota(jnp.int32, rt.shape, 1), SLAB_ROWS) + (offset - (HALO - GHOST))
    bit = 1
    while bit < EXT:
        rt = jnp.where((place & bit) != 0, pltpu.roll(rt, bit, 0), rt)
        bit *= 2
    level = lax.broadcasted_iota(jnp.int32, rt.shape, 0)
    outside = ((index == 0) & (level < GHOST)) | ((index == lax.axis_size("wave") - 1) & (level >= GHOST + SLAB_ROWS))
    return jnp.where(outside, 0.0, rt)


def pixel_kernel(offsets, starts, profile, band, frames, inverse_var, masked, t0, t1, f, rowmat, rowmat_t,
                 frames_s, inv_s, mask_s, sems, starts_s, profile_s, bands_s, side_sems, pad_s, start_s, band_s):
    fib = starts.shape[1]
    rows, width = t0.shape
    side_copies = [
        pltpu.make_async_copy(src, dst, side_sems.at[i])
        for i, (src, dst) in enumerate(((starts, starts_s), (profile, profile_s), (band, bands_s)))
    ]
    for c in side_copies:
        c.start()
    blocks = width // FB
    copies = []
    for b in range(blocks):
        cols = pl.ds(b * CB, CB)
        copies.append([
            pltpu.make_async_copy(src.at[:, :, cols], dst.at[:, :, cols], sems.at[b, i])
            for i, (src, dst) in enumerate(((inverse_var, inv_s), (masked, mask_s), (frames, frames_s)))
        ])
    for c in copies[0] + copies[1]:
        c.start()

    pad_s[...] = jnp.zeros_like(pad_s)
    start_s[...] = jnp.zeros_like(start_s)
    band_s[...] = jnp.zeros_like(band_s)
    for c in side_copies:
        c.wait()
    for i in range(rows // SLAB_ROWS):
        band_s[0:BAND, i * SLAB_ROWS : (i + 1) * SLAB_ROWS] = bands_s[i]
    for c in copies[2] + copies[3]:
        c.start()
    rt = row_matrix(band_s[...], offsets[0])
    rowmat_t[...] = rt
    rowmat[...] = rt.T
    for j in range(PW):
        pad_s[j : j + 1, 0:fib] = profile_s[j]
    start_s[0:1, 0:fib] = starts_s[...]
    lane = lax.broadcasted_iota(jnp.int32, (1, width), 1)
    jitter = start_s[0:1, :] - PITCH * lane
    base = pad_s[...]
    local = jnp.where(jitter == 0, base, 0.0)
    for d in range(1, 4):
        local = jnp.where(jitter == d, pltpu.roll(base, d, 0), local)
    low, high = local[0:8], local[8:16]
    nxt = pltpu.roll(low, width - 1, 1)

    def twice(x):
        return [jnp.concatenate([p.astype(F32)] * 2, 0).astype(BF16) for p in parts(x)]

    c_low, c_high = twice(low), twice(high)
    s_low, s_high = twice(low * low), twice(high * high)
    n_high = twice(high * nxt)
    zero = jnp.zeros((16, FB), BF16)
    lane = lax.broadcasted_iota(jnp.int32, (16, FB), 1) - lax.broadcasted_iota(jnp.int32, (16, FB), 0) // 8
    lane = lane.astype(F32).astype(BF16)
    edge = (lax.broadcasted_iota(jnp.int32, (16, FB), 1) == FB - 1) & (lax.broadcasted_iota(jnp.int32, (16, FB), 0) < 8)
    edge = edge.astype(F32).astype(BF16)

    def expand(b):
        cols = slice(b * FB, (b + 1) * FB)
        cl, ch = [x[:, cols] for x in c_low], [x[:, cols] for x in c_high]
        sl, sh = [x[:, cols] for x in s_low], [x[:, cols] for x in s_high]
        nh = [x[:, cols] for x in n_high]
        square, cross, plain = ([[], [], []] for _ in range(3))
        for t in range(CB // 16):
            on = lane == jnp.asarray(2 * t, BF16)
            after = lane == jnp.asarray(2 * t - 1, BF16)
            for i in range(3):
                square[i].append(jnp.where(on, sl[i], jnp.where(after, sh[i], zero)))
                cross[i].append(jnp.where(after, nh[i], zero))
                plain[i].append(jnp.where(on, cl[i], jnp.where(after, ch[i], zero)))
        return [[jnp.concatenate(x, 0) for x in group] for group in (square, cross, plain)]

    def products(w, v, square, cross, plain):
        pair = [jnp.concatenate([x, y], 1) for x, y in zip(square, cross)]
        t = mm(jnp.concatenate(w, 0), pair[0])
        g = mm(jnp.concatenate(w[0:2], 0), pair[1])
        t = t[0:rows] + t[rows : 2 * rows] + t[2 * rows :] + g[0:rows] + g[rows:] + mm(w[0], pair[2])
        g = mm(jnp.concatenate(v, 0), jnp.concatenate(plain[0:2], 1))
        g = g[0:rows] + g[rows : 2 * rows] + g[2 * rows :]
        g = g[:, 0:FB] + g[:, FB:] + mm(v[0], plain[2])
        return t[:, 0:FB], t[:, FB:], g

    for b in range(blocks):
        if b % 2 == 0:
            for c in copies[b] + copies[b + 1]:
                c.wait()
        at = slice(b * CB, (b + 1) * CB)
        w = (inv_s[:, :, at] * (1.0 - mask_s[:, :, at].astype(F32))).reshape(rows, CB)
        v = w * frames_s[:, :, at].reshape(rows, CB)
        w, v = parts(w), parts(v)
        tt, cc, gg = products(w, v, *expand(b))
        cols = slice(b * FB, (b + 1) * FB)
        t0[:, cols] = tt
        t1[:, cols] = cc
        f[:, cols] = gg
        if b > 0:
            cols = slice((b - 1) * FB, b * FB)
            below = jnp.zeros((FB - 16, FB), BF16)

            def tip(x):
                return jnp.concatenate([x[:, cols] * edge, below], 0)

            tips = [[tip(x) for x in group] for group in (s_high, n_high, c_high)]
            tt, cc, gg = products([x[:, 0:FB] for x in w], [x[:, 0:FB] for x in v], *tips)
            t0[:, cols] += tt
            t1[:, cols] += cc
            f[:, cols] += gg


def tri(t0, t1, u):
    width = u.shape[1]
    return t0 * u + t1 * pltpu.roll(u, width - 1, 1) + pltpu.roll(t1 * u, 1, 1)


def split(ext, parity, send_e, send_o, at):
    low, high = ext[0:HALF], ext[HALF:EXT]
    send_e[at : at + HALF, :] = jnp.where(parity == 0, high, low)
    send_o[at : at + HALF, :] = jnp.where(parity == 0, low, high)


def sides(e, o):
    index, last = lax.axis_index("wave"), lax.axis_size("wave") - 1
    even = lax.rem(index, 2) == 0
    low = jnp.where(index == 0, 0.0, jnp.where(even, o, e))
    return low, jnp.where(index == last, 0.0, jnp.where(even, e, o))


def joined(part, got_e, got_o, at):
    low, high = sides(got_e[at : at + HALF, :], got_o[at : at + HALF, :])
    return jnp.concatenate([part[0:HALF, :] + low, part[HALF:EXT, :] + high], 0)


def lanes_of(x):
    s = jnp.sum(x, axis=0, keepdims=True)
    total = s[:, 0:LANES]
    for i in range(1, x.shape[1] // LANES):
        total = total + s[:, i * LANES : (i + 1) * LANES]
    return total


def own(x):
    return x[GHOST : GHOST + SLAB_ROWS, :]


def first_kernel(flux, flux_e, flux_o, t0, t1, f, rowmat, rowmat_t, start_ext, part, send_e, send_o, ext_s):
    parity = lax.rem(lax.axis_index("wave"), 2)
    fib = flux.shape[1]
    ext_s[...] = jnp.zeros_like(ext_s)
    low, high = sides(flux_e[...], flux_o[...])
    ext_s[0:GHOST, 0:fib] = low[SLAB_ROWS - GHOST :]
    ext_s[GHOST : GHOST + SLAB_ROWS, 0:fib] = flux[...]
    ext_s[GHOST + SLAB_ROWS : EXT, 0:fib] = high[0:GHOST]
    r, rt = rowmat[...], rowmat_t[...]
    ext = ext_s[...]
    start_ext[...] = ext
    t = f[...] - tri(t0[...], t1[...], dot(r, ext))
    back = dot(rt, t)
    diag = dot(rt * rt, t0[...])
    part[0:EXT, :] = back
    part[EXT : 2 * EXT, :] = diag
    split(back, parity, send_e, send_o, 0)
    split(diag, parity, send_e, send_o, HALF)


def apply_rows(vec, rowmat, rowmat_t, t0, t1):
    u = dot(rowmat[...], vec)
    t = tri(t0[...], t1[...], u)
    return u, t, dot(rowmat_t[...], t)


def second_kernel(rowmat, rowmat_t, t0, t1, start_ext, part, got_e, got_o, diag, vec, mom, part_out, send_e, send_o):
    parity = lax.rem(lax.axis_index("wave"), 2)
    res = joined(part[0:EXT, :], got_e, got_o, 0) - RIDGE * start_ext[...]
    d = joined(part[EXT : 2 * EXT, :], got_e, got_o, HALF) + RIDGE
    p = res / d
    diag[...] = d
    vec[...] = p
    mom[...] = jnp.zeros_like(mom)
    mom[0:1, :] = lanes_of(own(p) * own(res))
    _, _, back = apply_rows(p, rowmat, rowmat_t, t0, t1)
    part_out[...] = back
    split(back, parity, send_e, send_o, 0)


def next_kernel(step, copies, rowmat, rowmat_t, t0, t1, diag, before, mom, part, got_e, got_o, vec, mom_out, part_out, send_e, send_o):
    parity = lax.rem(lax.axis_index("wave"), 2)
    prev = before[...]
    d = diag[...]
    image = joined(part, got_e, got_o, 0) + RIDGE * prev
    p = image / d - SHIFT * prev
    vec[...] = p
    scaled = own(d) * own(p)
    u, t, back = apply_rows(p, rowmat, rowmat_t, t0, t1)
    if copies:
        part_out[...] = own(back)
        low, high = back[0:GHOST], back[EXT - GHOST : EXT]
        send_e[...] = jnp.where(parity == 0, high, low)
        send_o[...] = jnp.where(parity == 0, low, high)
    else:
        part_out[...] = back
        split(back, parity, send_e, send_o, 0)
    moments = mom[...]
    row = lax.broadcasted_iota(jnp.int32, moments.shape, 0)
    new = [(2 * step - 1, lanes_of(scaled * own(prev))), (2 * step, lanes_of(scaled * own(p)))]
    if copies:
        new.append((2 * step + 1, lanes_of(u * t) + RIDGE * lanes_of(own(p) * own(p))))
    for i, value in new:
        moments = jnp.where(row == i, value, moments)
    if copies:
        mom_out[...] = jnp.broadcast_to(moments[None], mom_out.shape)
    else:
        mom_out[...] = moments


def coefficients(mom):
    mu = [mom[i : i + 1, :] for i in range(5)]
    nu = [mu[i + 1] + SHIFT * mu[i] for i in range(4)] + [mom[5:6, :]]

    def inner(p, w):
        total = None
        for i in range(len(p)):
            for j in range(len(p)):
                term = p[i] * p[j] * w[i + j]
                total = term if total is None else total + term
        return total

    one = jnp.ones_like(mu[0])
    rho, delta, energy = [one], [one], mu[0]
    chi = []
    for step in range(3):
        alpha = energy / inner(delta, nu)
        chi = [c + alpha * x for c, x in zip(chi + [0.0 * one], delta)]
        image = [SHIFT * x for x in delta] + [0.0 * one]
        image = [x + (delta[i - 1] if i else 0.0) for i, x in enumerate(image)]
        rho = [x - alpha * y for x, y in zip(rho + [0.0 * one], image)]
        if step < 2:
            fresh = inner(rho, mu)
            beta = fresh / energy
            delta = [x + beta * y for x, y in zip(rho, delta + [0.0 * one])]
            energy = fresh
    return chi, rho


def last_kernel(moms, diag, start_ext, p0, p1, p2, part, got_e, got_o, solution_ref, residual_ref):
    fib = solution_ref.shape[1]
    total = jnp.sum(moms[...], axis=0)
    total = jnp.broadcast_to(jnp.sum(total, axis=1, keepdims=True), total.shape)
    chi, rho = coefficients(total)
    width = diag.shape[1]

    def wide(c):
        return jnp.concatenate([c] * (width // LANES), 1)

    chi = [wide(c) for c in chi]
    rho = [wide(c) for c in rho]
    q0, q1, q2, d = own(p0), own(p1), own(p2), own(diag)
    low, high = sides(got_e[...], got_o[...])
    between = jnp.zeros((SLAB_ROWS - 2 * GHOST, width), F32)
    image = part[...] + jnp.concatenate([low, between, high] if SLAB_ROWS > 2 * GHOST else [low, high], 0) + RIDGE * q2
    x = own(start_ext) + chi[0] * q0 + chi[1] * q1 + chi[2] * q2
    r = d * (rho[0] * q0 + rho[1] * q1 + rho[2] * q2) + rho[3] * (image - SHIFT * (d * q2))
    solution_ref[...] = x[:, 0:fib]
    residual_ref[...] = r[:, 0:fib]


def partners(tiles, waves):
    even, odd = [], []
    for tile in range(tiles):
        for i in range(waves):
            here = tile * waves + i
            for found, other in ((even, i ^ 1), (odd, ((i + 1) ^ 1) - 1)):
                if 0 <= other < waves:
                    found.append((here, tile * waves + other))
                elif tile ^ 1 < tiles:
                    found.append((here, (tile ^ 1) * waves + i))
    return even, odd


def swap(send_o, odd, send_e, even):
    got_o = lax.ppermute(send_o, ("tile", "wave"), odd)
    got_e = lax.ppermute(send_e, ("tile", "wave"), even)
    return got_o, got_e


def local(frames, inverse_var, masked, psf_band, offsets, starts, profile, flux_start):
    waves = lax.axis_size("wave")
    fib = flux_start.shape[1]
    expo, slab, columns = frames.shape
    rows = expo * slab
    blocks = columns // CB
    width = blocks * FB
    even, odd = partners(lax.axis_size("tile"), waves)
    flux_o, flux_e = swap(flux_start, odd, flux_start, even)

    vm = pl.BlockSpec(memory_space=pltpu.VMEM)
    small = pltpu.CompilerParams(vmem_limit_bytes=VMEM_LIMIT)

    def shape(*dims):
        return jax.ShapeDtypeStruct(dims, F32)

    hb = pl.BlockSpec(memory_space=pltpu.HBM)
    sm = pl.BlockSpec(memory_space=pltpu.SMEM)
    raw = (offsets, starts, jnp.transpose(profile, (1, 0, 2)), jnp.transpose(psf_band, (0, 2, 1)), frames, inverse_var, masked)
    raw = [raw[0]] + [pltpu.with_memory_space_constraint(x, pltpu.HBM) for x in raw[1:]]
    t0, t1, f, rowmat, rowmat_t = pl.pallas_call(
        pixel_kernel,
        in_specs=[sm] + [hb] * 6,
        out_specs=[vm] * 5,
        out_shape=[shape(rows, width)] * 3 + [shape(rows, EXT), shape(EXT, rows)],
        scratch_shapes=[
            pltpu.VMEM(frames.shape, F32),
            pltpu.VMEM(frames.shape, F32),
            pltpu.VMEM(frames.shape, jnp.int32),
            pltpu.SemaphoreType.DMA((blocks, 3)),
            pltpu.VMEM((1, fib), jnp.int32),
            pltpu.VMEM((PW, 1, fib), F32),
            pltpu.VMEM((expo, BAND, slab), F32),
            pltpu.SemaphoreType.DMA((3,)),
            pltpu.VMEM((16, width), F32),
            pltpu.VMEM((8, width), jnp.int32),
            pltpu.VMEM((EXT, rows), F32),
        ],
        compiler_params=small,
        name="pixels",
    )(*raw)

    start_ext, part, send_e, send_o = pl.pallas_call(
        first_kernel,
        in_specs=[vm] * 8,
        out_specs=[vm] * 4,
        out_shape=[shape(EXT, width), shape(2 * EXT, width), shape(EXT, width), shape(EXT, width)],
        scratch_shapes=[pltpu.VMEM((EXT, width), F32)],
        compiler_params=small,
        name="first",
    )(flux_start, flux_e, flux_o, t0, t1, f, rowmat, rowmat_t)
    got_o, got_e = swap(send_o, odd, send_e, even)

    diag, p0, mom, part, send_e, send_o = pl.pallas_call(
        second_kernel,
        in_specs=[vm] * 8,
        out_specs=[vm] * 6,
        out_shape=[shape(EXT, width), shape(EXT, width), shape(8, LANES), shape(EXT, width), shape(HALF, width), shape(HALF, width)],
        compiler_params=small,
        name="second",
    )(rowmat, rowmat_t, t0, t1, start_ext, part, got_e, got_o)
    vectors = [p0]
    for step in (1, 2):
        got_o, got_e = swap(send_o, odd, send_e, even)
        copies = waves if step == 2 else 0
        mom_shape = shape(waves, 8, LANES) if copies else shape(8, LANES)
        vec, mom, part, send_e, send_o = pl.pallas_call(
            functools.partial(next_kernel, step, copies),
            in_specs=[vm] * 10,
            out_specs=[vm] * 5,
            out_shape=[shape(EXT, width), mom_shape, shape(EXT if step == 1 else slab, width), *[shape(HALF if step == 1 else GHOST, width)] * 2],
            compiler_params=small,
        )(rowmat, rowmat_t, t0, t1, diag, vectors[-1], mom, part, got_e, got_o)
        vectors.append(vec)
    got_o, got_e = swap(send_o, odd, send_e, even)
    moms = lax.all_to_all(mom, "wave", 0, 0)
    return tuple(
        pl.pallas_call(
            last_kernel,
            in_specs=[vm] * 9,
            out_specs=[vm] * 2,
            out_shape=[shape(slab, fib)] * 2,
            compiler_params=small,
        name="last",
        )(moms, diag, start_ext, *vectors, part, got_e, got_o)
    )


def solution(mesh):
    placed = (
        P(None, ("tile", "wave"), None),
        P(None, ("tile", "wave"), None),
        P(None, ("tile", "wave"), None),
        P(None, ("tile", "wave"), None),
        P(("tile", "wave")),
        P(("tile", "wave"), None),
        P(("tile", "wave"), None, None),
        P(("tile", "wave"), None),
    )
    return jax.shard_map(
        local,
        mesh=mesh,
        in_specs=placed,
        out_specs=(P(("tile", "wave"), None), P(("tile", "wave"), None)),
        check_vma=False,
    )
```

```python
import jax
import jax.numpy as jnp
from jax import lax
from jax.experimental import pallas as pl
from jax.experimental.pallas import tpu as pltpu
from jax.sharding import PartitionSpec as P


SLAB_ROWS = 32
HALO = 32
BAND = 16
PW = 12
PITCH = 8
RIDGE = 0.2
GHOST = 16
EXT = SLAB_ROWS + 2 * GHOST
HALF = EXT // 2
LANES = 128
FB = 128
CB = FB * PITCH
VMEM_LIMIT = 16 * 1024 * 1024
SHIFT = 14.0
F32 = jnp.float32
BF16 = jnp.bfloat16


def parts(x):
    high = x.astype(BF16)
    rest = x - high.astype(F32)
    mid = rest.astype(BF16)
    return high, mid, (rest - mid.astype(F32)).astype(BF16)


def mm(a, b):
    return lax.dot_general(a, b, (((1,), (0,)), ((), ())), preferred_element_type=F32)


def row_matrix(rt, offset):
    index = lax.axis_index("wave")
    place = lax.rem(lax.broadcasted_iota(jnp.int32, rt.shape, 1), SLAB_ROWS) + (offset - (HALO - GHOST))
    bit = 1
    while bit < EXT:
        rt = jnp.where((place & bit) != 0, pltpu.roll(rt, bit, 0), rt)
        bit *= 2
    level = lax.broadcasted_iota(jnp.int32, rt.shape, 0)
    outside = ((index == 0) & (level < GHOST)) | ((index == lax.axis_size("wave") - 1) & (level >= GHOST + SLAB_ROWS))
    return jnp.where(outside, 0.0, rt)


def pixel_kernel(offsets, starts, profile, band, frames, inverse_var, masked, t0, t1, f, rowmat, rowmat_t,
                 frames_s, inv_s, mask_s, sems, starts_s, profile_s, bands_s, side_sems, pad_s, start_s, band_s):
    fib = starts.shape[1]
    rows, width = t0.shape
    side_copies = [
        pltpu.make_async_copy(src, dst, side_sems.at[i])
        for i, (src, dst) in enumerate(((starts, starts_s), (profile, profile_s), (band, bands_s)))
    ]
    for c in side_copies:
        c.start()
    blocks = width // FB
    copies = []
    for b in range(blocks):
        cols = pl.ds(b * CB, CB)
        copies.append([
            pltpu.make_async_copy(src.at[:, :, cols], dst.at[:, :, cols], sems.at[b, i])
            for i, (src, dst) in enumerate(((inverse_var, inv_s), (masked, mask_s), (frames, frames_s)))
        ])
    for c in copies[0] + copies[1]:
        c.start()

    pad_s[...] = jnp.zeros_like(pad_s)
    start_s[...] = jnp.zeros_like(start_s)
    band_s[...] = jnp.zeros_like(band_s)
    for c in side_copies:
        c.wait()
    for i in range(rows // SLAB_ROWS):
        band_s[0:BAND, i * SLAB_ROWS : (i + 1) * SLAB_ROWS] = bands_s[i]
    for c in copies[2] + copies[3]:
        c.start()
    rt = row_matrix(band_s[...], offsets[0])
    rowmat_t[...] = rt
    rowmat[...] = rt.T
    for j in range(PW):
        pad_s[j : j + 1, 0:fib] = profile_s[j]
    start_s[0:1, 0:fib] = starts_s[...]
    lane = lax.broadcasted_iota(jnp.int32, (1, width), 1)
    jitter = start_s[0:1, :] - PITCH * lane
    base = pad_s[...]
    local = jnp.where(jitter == 0, base, 0.0)
    for d in range(1, 4):
        local = jnp.where(jitter == d, pltpu.roll(base, d, 0), local)
    low, high = local[0:8], local[8:16]
    nxt = pltpu.roll(low, width - 1, 1)

    def twice(x):
        return [jnp.concatenate([p.astype(F32)] * 2, 0).astype(BF16) for p in parts(x)]

    c_low, c_high = twice(low), twice(high)
    s_low, s_high = twice(low * low), twice(high * high)
    n_high = twice(high * nxt)
    zero = jnp.zeros((16, FB), BF16)
    lane = lax.broadcasted_iota(jnp.int32, (16, FB), 1) - lax.broadcasted_iota(jnp.int32, (16, FB), 0) // 8
    lane = lane.astype(F32).astype(BF16)
    edge = (lax.broadcasted_iota(jnp.int32, (16, FB), 1) == FB - 1) & (lax.broadcasted_iota(jnp.int32, (16, FB), 0) < 8)
    edge = edge.astype(F32).astype(BF16)

    def expand(b):
        cols = slice(b * FB, (b + 1) * FB)
        cl, ch = [x[:, cols] for x in c_low], [x[:, cols] for x in c_high]
        sl, sh = [x[:, cols] for x in s_low], [x[:, cols] for x in s_high]
        nh = [x[:, cols] for x in n_high]
        square, cross, plain = ([[], [], []] for _ in range(3))
        for t in range(CB // 16):
            on = lane == jnp.asarray(2 * t, BF16)
            after = lane == jnp.asarray(2 * t - 1, BF16)
            for i in range(3):
                square[i].append(jnp.where(on, sl[i], jnp.where(after, sh[i], zero)))
                cross[i].append(jnp.where(after, nh[i], zero))
                plain[i].append(jnp.where(on, cl[i], jnp.where(after, ch[i], zero)))
        return [[jnp.concatenate(x, 0) for x in group] for group in (square, cross, plain)]

    def products(w, v, square, cross, plain):
        pair = [jnp.concatenate([x, y], 1) for x, y in zip(square, cross)]
        t = mm(jnp.concatenate(w, 0), pair[0])
        g = mm(jnp.concatenate(w[0:2], 0), pair[1])
        t = t[0:rows] + t[rows : 2 * rows] + t[2 * rows :] + g[0:rows] + g[rows:] + mm(w[0], pair[2])
        g = mm(jnp.concatenate(v, 0), jnp.concatenate(plain[0:2], 1))
        g = g[0:rows] + g[rows : 2 * rows] + g[2 * rows :]
        g = g[:, 0:FB] + g[:, FB:] + mm(v[0], plain[2])
        return t[:, 0:FB], t[:, FB:], g

    for b in range(blocks):
        if b % 2 == 0:
            for c in copies[b] + copies[b + 1]:
                c.wait()
        at = slice(b * CB, (b + 1) * CB)
        w = (inv_s[:, :, at] * (1.0 - mask_s[:, :, at].astype(F32))).reshape(rows, CB)
        v = w * frames_s[:, :, at].reshape(rows, CB)
        w, v = parts(w), parts(v)
        tt, cc, gg = products(w, v, *expand(b))
        cols = slice(b * FB, (b + 1) * FB)
        t0[:, cols] = tt
        t1[:, cols] = cc
        f[:, cols] = gg
        if b > 0:
            cols = slice((b - 1) * FB, b * FB)
            below = jnp.zeros((FB - 16, FB), BF16)

            def tip(x):
                return jnp.concatenate([x[:, cols] * edge, below], 0)

            tips = [[tip(x) for x in group] for group in (s_high, n_high, c_high)]
            tt, cc, gg = products([x[:, 0:FB] for x in w], [x[:, 0:FB] for x in v], *tips)
            t0[:, cols] += tt
            t1[:, cols] += cc
            f[:, cols] += gg


def dot(a, b):
    m = a.shape[0]
    a, b = parts(a), parts(b)
    x = mm(jnp.concatenate(a, 0), b[0])
    y = mm(jnp.concatenate(a[0:2], 0), b[1])
    return mm(a[0], b[2]) + y[m:] + x[2 * m :] + y[0:m] + x[m : 2 * m] + x[0:m]


def tri(t0, t1, u):
    width = u.shape[1]
    return t0 * u + t1 * pltpu.roll(u, width - 1, 1) + pltpu.roll(t1 * u, 1, 1)


def split(ext, parity, send_e, send_o, at):
    low, high = ext[0:HALF], ext[HALF:EXT]
    send_e[at : at + HALF, :] = jnp.where(parity == 0, high, low)
    send_o[at : at + HALF, :] = jnp.where(parity == 0, low, high)


def sides(e, o):
    index, last = lax.axis_index("wave"), lax.axis_size("wave") - 1
    even = lax.rem(index, 2) == 0
    low = jnp.where(index == 0, 0.0, jnp.where(even, o, e))
    return low, jnp.where(index == last, 0.0, jnp.where(even, e, o))


def joined(part, got_e, got_o, at):
    low, high = sides(got_e[at : at + HALF, :], got_o[at : at + HALF, :])
    return jnp.concatenate([part[0:HALF, :] + low, part[HALF:EXT, :] + high], 0)


def lanes_of(x):
    s = jnp.sum(x, axis=0, keepdims=True)
    total = s[:, 0:LANES]
    for i in range(1, x.shape[1] // LANES):
        total = total + s[:, i * LANES : (i + 1) * LANES]
    return total


def own(x):
    return x[GHOST : GHOST + SLAB_ROWS, :]


def first_kernel(flux, flux_e, flux_o, t0, t1, f, rowmat, rowmat_t, start_ext, part, send_e, send_o, ext_s):
    parity = lax.rem(lax.axis_index("wave"), 2)
    fib = flux.shape[1]
    ext_s[...] = jnp.zeros_like(ext_s)
    low, high = sides(flux_e[...], flux_o[...])
    ext_s[0:GHOST, 0:fib] = low[SLAB_ROWS - GHOST :]
    ext_s[GHOST : GHOST + SLAB_ROWS, 0:fib] = flux[...]
    ext_s[GHOST + SLAB_ROWS : EXT, 0:fib] = high[0:GHOST]
    r, rt = rowmat[...], rowmat_t[...]
    ext = ext_s[...]
    start_ext[...] = ext
    t = f[...] - tri(t0[...], t1[...], dot(r, ext))
    back = dot(rt, t)
    diag = dot(rt * rt, t0[...])
    part[0:EXT, :] = back
    part[EXT : 2 * EXT, :] = diag
    split(back, parity, send_e, send_o, 0)
    split(diag, parity, send_e, send_o, HALF)


def apply_rows(vec, rowmat, rowmat_t, t0, t1):
    u = dot(rowmat[...], vec)
    t = tri(t0[...], t1[...], u)
    return u, t, dot(rowmat_t[...], t)


def second_kernel(rowmat, rowmat_t, t0, t1, start_ext, part, got_e, got_o, diag, vec, mom, part_out, send_e, send_o):
    parity = lax.rem(lax.axis_index("wave"), 2)
    res = joined(part[0:EXT, :], got_e, got_o, 0) - RIDGE * start_ext[...]
    d = joined(part[EXT : 2 * EXT, :], got_e, got_o, HALF) + RIDGE
    p = res / d
    diag[...] = d
    vec[...] = p
    mom[...] = jnp.zeros_like(mom)
    mom[0:1, :] = lanes_of(own(p) * own(res))
    _, _, back = apply_rows(p, rowmat, rowmat_t, t0, t1)
    part_out[...] = back
    split(back, parity, send_e, send_o, 0)


def next_vector(diag, before, part, got_e, got_o):
    prev = before[...]
    d = diag[...]
    image = joined(part, got_e, got_o, 0) + RIDGE * prev
    p = image / d - SHIFT * prev
    scaled = own(d) * own(p)
    return p, [lanes_of(scaled * own(prev)), lanes_of(scaled * own(p))]


def placed_rows(moments, first, new):
    row = lax.broadcasted_iota(jnp.int32, moments.shape, 0)
    for i, value in enumerate(new):
        moments = jnp.where(row == first + i, value, moments)
    return moments


def third_kernel(rowmat, rowmat_t, t0, t1, diag, before, mom, part, got_e, got_o, vec, mom_out, part_out, send_e, send_o):
    parity = lax.rem(lax.axis_index("wave"), 2)
    p, new = next_vector(diag, before, part, got_e, got_o)
    vec[...] = p
    _, _, back = apply_rows(p, rowmat, rowmat_t, t0, t1)
    part_out[...] = back
    split(back, parity, send_e, send_o, 0)
    mom_out[...] = placed_rows(mom[...], 1, new)


def fourth_kernel(rowmat, t0, t1, diag, before, mom, part, got_e, got_o, vec, mom_out, rows_out):
    p, new = next_vector(diag, before, part, got_e, got_o)
    vec[...] = p
    u = dot(rowmat[...], p)
    t = tri(t0[...], t1[...], u)
    rows_out[...] = t
    new.append(lanes_of(u * t) + RIDGE * lanes_of(own(p) * own(p)))
    mom_out[...] = jnp.broadcast_to(placed_rows(mom[...], 3, new)[None], mom_out.shape)


def image_kernel(rowmat_t, rows_in, part_out, send_e, send_o):
    parity = lax.rem(lax.axis_index("wave"), 2)
    back = dot(rowmat_t[...], rows_in[...])
    part_out[...] = own(back)
    low, high = back[0:GHOST], back[EXT - GHOST : EXT]
    send_e[...] = jnp.where(parity == 0, high, low)
    send_o[...] = jnp.where(parity == 0, low, high)


def coefficients(mom):
    mu = [mom[i : i + 1, :] for i in range(5)]
    nu = [mu[i + 1] + SHIFT * mu[i] for i in range(4)] + [mom[5:6, :]]

    def inner(p, w):
        total = None
        for i in range(len(p)):
            for j in range(len(p)):
                term = p[i] * p[j] * w[i + j]
                total = term if total is None else total + term
        return total

    one = jnp.ones_like(mu[0])
    rho, delta, energy = [one], [one], mu[0]
    chi = []
    for step in range(3):
        alpha = energy / inner(delta, nu)
        chi = [c + alpha * x for c, x in zip(chi + [0.0 * one], delta)]
        image = [SHIFT * x for x in delta] + [0.0 * one]
        image = [x + (delta[i - 1] if i else 0.0) for i, x in enumerate(image)]
        rho = [x - alpha * y for x, y in zip(rho + [0.0 * one], image)]
        if step < 2:
            fresh = inner(rho, mu)
            beta = fresh / energy
            delta = [x + beta * y for x, y in zip(rho, delta + [0.0 * one])]
            energy = fresh
    return chi, rho


def last_kernel(moms, diag, start_ext, p0, p1, p2, part, got_e, got_o, solution_ref, residual_ref):
    fib = solution_ref.shape[1]
    total = jnp.sum(moms[...], axis=0)
    total = jnp.broadcast_to(jnp.sum(total, axis=1, keepdims=True), total.shape)
    chi, rho = coefficients(total)
    width = diag.shape[1]

    def wide(c):
        return jnp.concatenate([c] * (width // LANES), 1)

    chi = [wide(c) for c in chi]
    rho = [wide(c) for c in rho]
    q0, q1, q2, d = own(p0), own(p1), own(p2), own(diag)
    low, high = sides(got_e[...], got_o[...])
    between = jnp.zeros((SLAB_ROWS - 2 * GHOST, width), F32)
    image = part[...] + jnp.concatenate([low, between, high] if SLAB_ROWS > 2 * GHOST else [low, high], 0) + RIDGE * q2
    x = own(start_ext) + chi[0] * q0 + chi[1] * q1 + chi[2] * q2
    r = d * (rho[0] * q0 + rho[1] * q1 + rho[2] * q2) + rho[3] * (image - SHIFT * (d * q2))
    solution_ref[...] = x[:, 0:fib]
    residual_ref[...] = r[:, 0:fib]


def partners(tiles, waves):
    even, odd = [], []
    for tile in range(tiles):
        for i in range(waves):
            here = tile * waves + i
            for found, other in ((even, i ^ 1), (odd, ((i + 1) ^ 1) - 1)):
                if 0 <= other < waves:
                    found.append((here, tile * waves + other))
                elif tile ^ 1 < tiles:
                    found.append((here, (tile ^ 1) * waves + i))
    return even, odd


def swap(send_o, odd, send_e, even):
    got_o = lax.ppermute(send_o, ("tile", "wave"), odd)
    got_e = lax.ppermute(send_e, ("tile", "wave"), even)
    return got_o, got_e


def local(frames, inverse_var, masked, psf_band, offsets, starts, profile, flux_start):
    waves = lax.axis_size("wave")
    fib = flux_start.shape[1]
    expo, slab, columns = frames.shape
    rows = expo * slab
    blocks = columns // CB
    width = blocks * FB
    even, odd = partners(lax.axis_size("tile"), waves)
    flux_o, flux_e = swap(flux_start, odd, flux_start, even)

    vm = pl.BlockSpec(memory_space=pltpu.VMEM)
    small = pltpu.CompilerParams(vmem_limit_bytes=VMEM_LIMIT)

    def shape(*dims):
        return jax.ShapeDtypeStruct(dims, F32)

    hb = pl.BlockSpec(memory_space=pltpu.HBM)
    sm = pl.BlockSpec(memory_space=pltpu.SMEM)
    raw = (offsets, starts, jnp.transpose(profile, (1, 0, 2)), jnp.transpose(psf_band, (0, 2, 1)), frames, inverse_var, masked)
    raw = [raw[0]] + [pltpu.with_memory_space_constraint(x, pltpu.HBM) for x in raw[1:]]
    t0, t1, f, rowmat, rowmat_t = pl.pallas_call(
        pixel_kernel,
        in_specs=[sm] + [hb] * 6,
        out_specs=[vm] * 5,
        out_shape=[shape(rows, width)] * 3 + [shape(rows, EXT), shape(EXT, rows)],
        scratch_shapes=[
            pltpu.VMEM(frames.shape, F32),
            pltpu.VMEM(frames.shape, F32),
            pltpu.VMEM(frames.shape, jnp.int32),
            pltpu.SemaphoreType.DMA((blocks, 3)),
            pltpu.VMEM((1, fib), jnp.int32),
            pltpu.VMEM((PW, 1, fib), F32),
            pltpu.VMEM((expo, BAND, slab), F32),
            pltpu.SemaphoreType.DMA((3,)),
            pltpu.VMEM((16, width), F32),
            pltpu.VMEM((8, width), jnp.int32),
            pltpu.VMEM((EXT, rows), F32),
        ],
        compiler_params=small,
        name="pixels",
    )(*raw)

    start_ext, part, send_e, send_o = pl.pallas_call(
        first_kernel,
        in_specs=[vm] * 8,
        out_specs=[vm] * 4,
        out_shape=[shape(EXT, width), shape(2 * EXT, width), shape(EXT, width), shape(EXT, width)],
        scratch_shapes=[pltpu.VMEM((EXT, width), F32)],
        compiler_params=small,
        name="first",
    )(flux_start, flux_e, flux_o, t0, t1, f, rowmat, rowmat_t)
    got_o, got_e = swap(send_o, odd, send_e, even)

    diag, p0, mom, part, send_e, send_o = pl.pallas_call(
        second_kernel,
        in_specs=[vm] * 8,
        out_specs=[vm] * 6,
        out_shape=[shape(EXT, width), shape(EXT, width), shape(8, LANES), shape(EXT, width), shape(HALF, width), shape(HALF, width)],
        compiler_params=small,
        name="second",
    )(rowmat, rowmat_t, t0, t1, start_ext, part, got_e, got_o)
    got_o, got_e = swap(send_o, odd, send_e, even)
    p1, mom, part, send_e, send_o = pl.pallas_call(
        third_kernel,
        in_specs=[vm] * 10,
        out_specs=[vm] * 5,
        out_shape=[shape(EXT, width), shape(8, LANES), shape(EXT, width), shape(HALF, width), shape(HALF, width)],
        compiler_params=small,
        name="third",
    )(rowmat, rowmat_t, t0, t1, diag, p0, mom, part, got_e, got_o)
    got_o, got_e = swap(send_o, odd, send_e, even)
    p2, mom, image_rows = pl.pallas_call(
        fourth_kernel,
        in_specs=[vm] * 9,
        out_specs=[vm] * 3,
        out_shape=[shape(EXT, width), shape(waves, 8, LANES), shape(rows, width)],
        compiler_params=small,
        name="fourth",
    )(rowmat, t0, t1, diag, p1, mom, part, got_e, got_o)
    moms = lax.all_to_all(mom, "wave", 0, 0)
    part, send_e, send_o = pl.pallas_call(
        image_kernel,
        in_specs=[vm] * 2,
        out_specs=[vm] * 3,
        out_shape=[shape(slab, width), shape(GHOST, width), shape(GHOST, width)],
        compiler_params=small,
        name="image",
    )(rowmat_t, image_rows)
    got_o, got_e = swap(send_o, odd, send_e, even)
    vectors = (p0, p1, p2)
    return tuple(
        pl.pallas_call(
            last_kernel,
            in_specs=[vm] * 9,
            out_specs=[vm] * 2,
            out_shape=[shape(slab, fib)] * 2,
            compiler_params=small,
        name="last",
        )(moms, diag, start_ext, *vectors, part, got_e, got_o)
    )


def solution(mesh):
    placed = (
        P(None, ("tile", "wave"), None),
        P(None, ("tile", "wave"), None),
        P(None, ("tile", "wave"), None),
        P(None, ("tile", "wave"), None),
        P(("tile", "wave")),
        P(("tile", "wave"), None),
        P(("tile", "wave"), None, None),
        P(("tile", "wave"), None),
    )
    return jax.shard_map(
        local,
        mesh=mesh,
        in_specs=placed,
        out_specs=(P(("tile", "wave"), None), P(("tile", "wave"), None)),
        check_vma=False,
    )
```
